32 devices in a mesh: section: 4 (over y, x), stem: 8 (over z, core).
Axes of the slice: x: 2, y: 2, z: 4, core: 2. Of those that a mesh axis runs over, the one named last changes fastest.
Arguments:
- bitstrings: int32 [4, 4, 32, 3], P('section'), may hold values 0 or 1
- boundary: float32 [2, 2048], replicated, may hold values from -6 to 6
- stem_tensor: float32 [4, 2, 2048, 8, 2048], P('section', None, 'stem'), may hold values from -0.09375 to 0.09375
- probe_vectors: float32 [4, 2, 2048], P('section'), may hold values from -0.09375 to 0.09375
- inbound_permutations: int32 [4, 2048], replicated, may hold values from 0 to 2047, each once within a row
Outputs:
- amplitudes: float32 [4, 2, 4, 32], P('section')
The draws below stay inside these ranges and needn't reach their ends.
Inputs may be any that keep to these rules, and one draw needn't show every extreme that they name: `inbound_permutations`: each row of relabeling names every number of 0 to 2047 once.
All inputs are finite; a program needn't handle non-finite values. No bound on the sum of `bitstrings` on one device may be relied on, other than what follows from the above.
Results may differ from the reference program's by a relative error of at most 0.0003.
Values sent between devices are 32-bit elements; how exact they have to be, the bound alone decides.
A program may use at most 128 MiB of HBM per device.

```python
import jax
import jax.numpy as jnp
from jax import lax

K = 2048
QS = 3
P_SIZE = 8
B = 32
M = 4
N_SECTION = 4


def touch_ends(array, rng, least, top_value):
    longest = array.shape.index(max(array.shape))
    spots = []
    for shift in (0, 1):
        where = [jax.random.randint(jax.random.fold_in(rng, axis), (), 0, length) for axis, length in enumerate(array.shape)]
        where[longest] = (where[longest] + shift) % array.shape[longest]
        spots.append(tuple(where))
    return array.at[spots[0]].set(least).at[spots[1]].set(top_value)


def levels(stream_key, dims, cuts, low, top_value):
    gain = 1.0
    for dim, shards_of in cuts:
        draws = jax.random.uniform(jax.random.fold_in(jax.random.fold_in(stream_key, 6), dim), (shards_of,), jnp.float32, low / len(cuts), top_value / len(cuts))
        gain = gain * jnp.repeat(jnp.exp(draws), dims[dim] // shards_of).reshape((-1,) + (1,) * (len(dims) - 1 - dim))
    return gain


def scatter_about(rng, dims, spread, limit, pieces=(), kind=jnp.bfloat16):
    values = spread * jax.random.normal(rng, dims, jnp.float32)
    if pieces:
        values = values * levels(rng, dims, pieces, -0.22, 0.18)
    return jnp.clip(values, -limit, limit).astype(kind)


def setup_inputs(seed: int = 0) -> dict:
    key_of = jax.random.split(jax.random.key(seed), 6)
    bitstrings = touch_ends((jax.random.randint(key_of[0], (N_SECTION, M, B, QS), 0, 2) < 1).astype(jnp.int32), jax.random.fold_in(key_of[0], 1), 0, 1)
    boundary = scatter_about(key_of[1], (2, K), 1.0, 6.0, (), jnp.float32)
    stem_tensor = scatter_about(key_of[2], (N_SECTION, 2, K, P_SIZE, K), (2 * K) ** -0.5, 0.09375, ((0, 4), (2, 8)), jnp.float32)
    probe_vectors = scatter_about(key_of[3], (N_SECTION, 2, K), (2 * K) ** -0.5, 0.09375, ((0, 4),), jnp.float32)
    inbound_permutations = jax.vmap(lambda own: jax.random.permutation(own, K))(jax.random.split(key_of[4], N_SECTION)).reshape((N_SECTION, K)).astype(jnp.int32)
    return {"bitstrings": bitstrings, "boundary": boundary, "stem_tensor": stem_tensor, "probe_vectors": probe_vectors, "inbound_permutations": inbound_permutations}


def reference(bitstrings, boundary, stem_tensor, probe_vectors, inbound_permutations):
    powers = (2 ** jnp.arange(QS)).astype(jnp.int32)
    configuration_line = jnp.sum(bitstrings * powers, axis=-1).astype(jnp.int32)
    running_partial_vector = jnp.broadcast_to(boundary[:, None, None, :], (2, M, B, K)).astype(jnp.float32)
    collected = []
    for segment_ordinal in range(N_SECTION):
        reordered_factor = jnp.take(running_partial_vector, inbound_permutations[segment_ordinal], axis=3)
        flat_real = stem_tensor[segment_ordinal, 0].reshape(K * P_SIZE, K)
        flat_imag = stem_tensor[segment_ordinal, 1].reshape(K * P_SIZE, K)

        def forward_group_move(pair):
            vectors, pattern = pair
            onehot = (jnp.arange(P_SIZE).astype(jnp.int32)[None, :] == pattern[:, None]).astype(jnp.float32)
            expanded = (vectors[:, :, :, None] * onehot[None, :, None, :]).reshape(2 * B, K * P_SIZE)
            prod_real = jnp.dot(expanded, flat_real, precision=lax.Precision.HIGHEST)
            prod_imag = jnp.dot(expanded, flat_imag, precision=lax.Precision.HIGHEST)
            out_real = prod_real[:B] - prod_imag[B:]
            out_imag = prod_imag[:B] + prod_real[B:]
            return jnp.stack([out_real, out_imag])

        permuted_entries = lax.map(forward_group_move, (jnp.transpose(reordered_factor, (1, 0, 2, 3)), configuration_line[segment_ordinal]))
        running_partial_vector = jnp.transpose(permuted_entries, (1, 0, 2, 3))
        probe_re = probe_vectors[segment_ordinal, 0]
        probe_im = probe_vectors[segment_ordinal, 1]
        amp_real = jnp.dot(running_partial_vector[0], probe_re, precision=lax.Precision.HIGHEST) - jnp.dot(running_partial_vector[1], probe_im, precision=lax.Precision.HIGHEST)
        amp_imag = jnp.dot(running_partial_vector[0], probe_im, precision=lax.Precision.HIGHEST) + jnp.dot(running_partial_vector[1], probe_re, precision=lax.Precision.HIGHEST)
        collected.append(jnp.stack([amp_real, amp_imag]))
    return jnp.stack(collected)
```

```python
import functools

import jax
import jax.numpy as jnp
from jax import lax
from jax.experimental import pallas as pl
from jax.experimental.pallas import tpu as pltpu
from jax.sharding import PartitionSpec as P

MESH = pl.DeviceIdType.MESH
VMEM = pl.BlockSpec(memory_space=pltpu.VMEM)
SMEM = pl.BlockSpec(memory_space=pltpu.SMEM)
ANY = pl.BlockSpec(memory_space=pl.ANY)
F32, BF16 = jnp.float32, jnp.bfloat16
LANES = 128
SLOTS = 4
STEP = 16
GROUPS = 4


def send(src, dst, send_sem, recv_sem, target):
    return pltpu.make_async_remote_copy(
        src_ref=src, dst_ref=dst, send_sem=send_sem, recv_sem=recv_sem, device_id=target, device_id_type=MESH
    )


def nn(a, b):
    return jnp.dot(a, b, preferred_element_type=F32)


def nt(a, b):
    return lax.dot_general(a, b, (((1,), (1,)), ((), ())), preferred_element_type=F32)


def halves(x):
    hi = x.astype(BF16)
    return hi, (x - hi.astype(F32)).astype(BF16)


def stacked(x):
    return jnp.concatenate(halves(x), axis=0)


def folded(y):
    n = y.shape[0] // 2
    return y[:n] + y[n:]


def turned(x):
    n = x.shape[0] // 2
    return jnp.concatenate([-x[n:], x[:n]], axis=0)


def rows_of(shape):
    return lax.broadcasted_iota(jnp.int32, shape, 0)


def lanes_of(shape):
    return lax.broadcasted_iota(jnp.int32, shape, 1)


def kernel(
    S, R, rows, P_, K, count,
    bits_ref, bnd_ref, perm0_ref, perm_ref, probe_ref, stem_ref, out_ref,
    buf, hl, place, wide, own, sets, set_own, uland, vland, snd, big, bighl, mine, other, xland, wown, wland, v2land,
    gram, part, fin, total,
    load_sem, set_s, set_r, u_s, u_r, v_s, v_r, v2_s, v2_r, x_s, x_r, w_s, w_r, f_s, f_r,
):
    me_s, me_r = lax.axis_index("section"), lax.axis_index("stem")
    half = R // 2
    parity = me_r % 2
    partner = me_r + 1 - 2 * parity
    chunks = rows // STEP
    C2 = 2 * P_
    tiles = K // LANES

    def load(i):
        slot = i % SLOTS
        for j in range(tiles):
            pltpu.make_async_copy(
                stem_ref.at[:, pl.ds(i * STEP * P_, STEP * P_), pl.ds(j * LANES, LANES)],
                buf.at[slot, j],
                load_sem.at[slot],
            ).start()

    def loaded(slot):
        pltpu.make_async_copy(buf.at[slot], buf.at[slot], load_sem.at[slot]).wait()

    for i in range(min(SLOTS, chunks)):
        load(i)

    barrier = pltpu.get_barrier_semaphore()
    for e in range(S):
        for d in range(R):
            if e + d:
                pl.semaphore_signal(
                    barrier, inc=1, device_id=((me_s + e) % S, (me_r + d) % R), device_id_type=MESH
                )

    qubits, micro, batch = bits_ref.shape
    codes = bits_ref[0].astype(F32)
    for q in range(1, qubits):
        codes = codes + float(2**q) * bits_ref[q].astype(F32)
    spread = jnp.zeros((8, count), F32)
    for m in range(micro):
        shift = (lanes_of((batch, count)) == rows_of((batch, count)) + m * batch).astype(F32).astype(BF16)
        spread = spread + nn(jnp.broadcast_to(codes[m : m + 1, :], (8, batch)).astype(BF16), shift)
    set_own[...] = spread

    own[...] = jnp.zeros_like(own)
    wide[...] = jnp.zeros_like(wide)

    blocks = tiles // chunks

    def build(i):
        for b in range(blocks):
            start = pl.multiple_of((i * blocks + b) * LANES, LANES)
            every = perm_ref[:, pl.ds(start, LANES)].astype(F32)
            row = jnp.sum(jnp.where(rows_of((S, LANES)) == (me_s + 1) % S, every, 0.0), axis=0, keepdims=True)
            col = jnp.broadcast_to(row, (LANES, LANES)).T
            for j in range(tiles):
                target = (lanes_of((LANES, LANES)) + j * LANES).astype(F32)
                place[pl.ds(start, LANES), j * LANES : (j + 1) * LANES] = (col == target).astype(F32).astype(BF16)

    def first(i, slot):
        scal = []
        for k in range(STEP):
            at = perm0_ref[0, me_r * rows + i * STEP + k]
            scal.append((bnd_ref[0, at], bnd_ref[1, at]))
        span = 4
        for g in range(tiles // span):
            cols = [slice((g * span + t) * LANES, (g * span + t + 1) * LANES) for t in range(span)]
            a = [wide[0:P_, js] for js in cols]
            b = [wide[P_:C2, js] for js in cols]
            for k in range(STEP):
                br, bi = scal[k]
                for t in range(span):
                    tr = buf[slot, g * span + t, 0, k * P_ : (k + 1) * P_, :]
                    ti = buf[slot, g * span + t, 1, k * P_ : (k + 1) * P_, :]
                    a[t] = a[t] + (br * tr - bi * ti)
                    b[t] = b[t] + (br * ti + bi * tr)
            for t in range(span):
                wide[0:P_, cols[t]] = a[t]
                wide[P_:C2, cols[t]] = b[t]

    def against_probe(i, slot):
        width = min(rows, LANES)
        block = pl.multiple_of((i * STEP // width) * width, width)
        lane = lanes_of((P_, width))
        at = pl.ds(block, width) if rows > width else slice(None)
        a, b = own[0:P_, at], own[P_:C2, at]
        for k in range(STEP):
            ar = jnp.zeros((P_, LANES), F32)
            ai = jnp.zeros((P_, LANES), F32)
            for j in range(tiles):
                js = slice(j * LANES, (j + 1) * LANES)
                tr = buf[slot, j, 0, k * P_ : (k + 1) * P_, :]
                ti = buf[slot, j, 1, k * P_ : (k + 1) * P_, :]
                pr, pi = wide[0:P_, js], wide[P_:C2, js]
                ar = ar + (tr * pr - ti * pi)
                ai = ai + (tr * pi + ti * pr)
            hit = lane == (i * STEP + k - block)
            a = jnp.where(hit, jnp.sum(ar, axis=1, keepdims=True), a)
            b = jnp.where(hit, jnp.sum(ai, axis=1, keepdims=True), b)
        own[0:P_, at] = a
        own[P_:C2, at] = b

    def split(i, slot):
        at = pl.ds(pl.multiple_of(i * STEP, STEP), STEP)

        def column(j, carry):
            js = pl.ds(pl.multiple_of(j * LANES, LANES), LANES)
            for c in range(2):
                for p in range(P_):
                    hi, lo = halves(buf[slot, j, c, pl.ds(p, STEP, P_), :])
                    hl[c, 0, p, at, js] = hi
                    hl[c, 1, p, at, js] = lo
            return carry

        lax.fori_loop(0, tiles, column, 0)

    @pl.when(me_s >= 2)
    def _():
        wide[0:P_, :] = jnp.broadcast_to(probe_ref[0:1, :], (P_, K))
        wide[P_:C2, :] = jnp.broadcast_to(probe_ref[1:2, :], (P_, K))

    def stream(i, carry):
        slot = i % SLOTS
        loaded(slot)

        @pl.when(me_s == 0)
        def _():
            build(i)
            first(i, slot)

        @pl.when(me_s == 1)
        def _():
            build(i)
            split(i, slot)

        @pl.when(me_s == 2)
        def _():
            build(i)
            split(i, slot)
            against_probe(i, slot)

        @pl.when(me_s == 3)
        def _():
            against_probe(i, slot)

        @pl.when(i + SLOTS < chunks)
        def _():
            load(i + SLOTS)

        return carry

    lax.fori_loop(0, chunks, stream, 0)
    pl.semaphore_wait(barrier, S * R - 1)

    def set_copy():
        return send(set_own, sets.at[me_s], set_s.at[0], set_r.at[me_s], (1, me_r))

    def set_wait(s):
        send(sets.at[s], sets.at[s], set_s.at[0], set_r.at[s], (0, me_r)).wait_recv()

    @pl.when(me_s != 1)
    def _():
        set_copy().start()

    def finals(section, lo):
        return [
            send(part, fin.at[me_r], f_s.at[e * R + d], f_r.at[me_r], (section + e, (me_r + d) % R))
            for e in range(lo)
            for d in range(R)
            if e + d
        ]

    setting = lambda s: sets[s, 0:1, :].astype(jnp.int32)

    @pl.when(me_s == 0)
    def _():
        u = stacked(wide[...])

        def piece(d, carry):
            to = (me_r + d) % R
            snd[to] = folded(nt(u, place[pl.ds(pl.multiple_of(to * rows, rows), rows), :]))
            send(snd.at[to], uland.at[me_r], u_s.at[to], u_r.at[me_r], (1, to)).start()
            return carry

        lax.fori_loop(0, R, piece, 0)
        ur, ui = wide[0:P_, :], wide[P_:C2, :]
        pr, pi = probe_ref[0:1, :], probe_ref[1:2, :]
        hit = rows_of((P_, count)) == set_own[0:1, :].astype(jnp.int32)
        re = jnp.sum(ur * pr - ui * pi, axis=1, keepdims=True)
        im = jnp.sum(ur * pi + ui * pr, axis=1, keepdims=True)
        part[...] = jnp.zeros_like(part)
        part[0:1, :] = jnp.sum(jnp.where(hit, re, 0.0), axis=0, keepdims=True)
        part[1:2, :] = jnp.sum(jnp.where(hit, im, 0.0), axis=0, keepdims=True)
        fin[me_r] = part[...]
        for copy in finals(0, 1):
            copy.start()

    @pl.when(me_s == 3)
    def _():
        for d in range(R):
            to = (me_r + d) % R
            send(own, vland.at[me_r], v_s.at[d], v_r.at[me_r], (2, to)).start()

    def w_copy(g, t):
        to = (me_r + 2 * t) % R
        n = wown.shape[0] // GROUPS
        at = pl.ds(pl.multiple_of(g * n, n), n)
        return send(
            wown.at[at], wland.at[me_r // 2, at], w_s.at[g * half + t], w_r.at[(me_r // 2) * GROUPS + g], (1, to)
        )

    def v2_copy(t):
        to = (me_r + 2 * t) % R
        return send(own, v2land.at[me_r // 2], v2_s.at[t], v2_r.at[me_r // 2], (1, to))

    @pl.when(me_s == 2)
    def _():
        for t in range(half):
            v2_copy(t).start()
        for r in range(R):
            send(vland.at[r], vland.at[r], v_s.at[0], v_r.at[r], (3, me_r)).wait_recv()
        y = nn(stacked(vland[0]), place[0:rows, :])
        for r in range(1, R):
            y = y + nn(stacked(vland[r]), place[r * rows : (r + 1) * rows, :])
        hi, lo = y[:C2], y[C2:]
        straight = jnp.concatenate([hi, lo], axis=0).astype(BF16)
        crossed = jnp.concatenate([turned(hi), turned(lo)], axis=0).astype(BF16)

        def group(g, carry):
            for e in range(P_ // GROUPS):
                p = g * (P_ // GROUPS) + e
                z = nt(straight, hl[0, 0, p]) + nt(crossed, hl[1, 0, p])
                z = z + nt(straight, hl[0, 1, p]) + nt(crossed, hl[1, 1, p])
                wown[pl.ds(pl.multiple_of(p * C2, C2), C2), :] = folded(z)
            for t in range(half):
                w_copy(g, t).start()
            return carry

        lax.fori_loop(0, GROUPS, group, 0)

    @pl.when(me_s == 1)
    def _():
        for r in range(R):
            send(uland.at[r], uland.at[r], u_s.at[0], u_r.at[r], (0, me_r)).wait_recv()
        x = uland[0]
        for r in range(1, R):
            x = x + uland[r]
        straight, crossed = stacked(x), stacked(turned(x))

        def front(p, carry):
            z = nn(straight, hl[0, 0, p]) + nn(crossed, hl[1, 0, p])
            z = z + nn(straight, hl[0, 1, p]) + nn(crossed, hl[1, 1, p])
            hi, lo = halves(folded(z))
            at = pl.multiple_of(p * C2, C2)
            bighl[pl.ds(at, C2), :] = hi
            bighl[pl.ds(pl.multiple_of(P_ * C2 + p * C2, C2), C2), :] = lo
            return carry

        lax.fori_loop(0, P_, front, 0)
        n = P_ * C2

        def shuffled(q):
            return folded(nt(bighl[...], place[pl.ds(pl.multiple_of(q * rows, rows), rows), :]))

        def x_copy(t):
            return send(other.at[t], xland.at[t], x_s.at[t], x_r.at[t], (1, partner))

        def give(t, carry):
            other[t] = shuffled(2 * t + 1 - parity)
            x_copy(t).start()
            return carry

        def keep(t, carry):
            mine[t] = shuffled(2 * t + parity)
            return carry

        lax.fori_loop(0, half, give, 0)
        lax.fori_loop(0, half, keep, 0)
        probes = jnp.concatenate([probe_ref[...], jnp.zeros((6, K), F32)], axis=0)
        g1 = folded(nt(stacked(probes), bighl[...]))
        gram[n + C2 : n + C2 + 8, :] = g1[:, :n] + g1[:, n:]
        sets[1] = set_own[...]
        for s in (0, 2, 3):
            set_wait(s)
        hits = [rows_of((n, count)) == setting(1) * C2 + c * P_ + setting(0) for c in range(2)]
        pick = jnp.concatenate([h.astype(F32) for h in hits], axis=1).astype(BF16)

        g2 = jnp.zeros((2 * C2, 2 * n), F32)
        for t in range(half):
            x_copy(t).wait_recv()
            both = mine[t] + xland[t]
            hi, lo = halves(both)
            big[t, 0:n, :] = hi
            big[t, n : 2 * n, :] = lo
            send(v2land.at[t], v2land.at[t], v2_s.at[0], v2_r.at[t], (2, me_r)).wait_recv()
            g2 = g2 + nt(stacked(v2land[t]), big[t])
        g2 = folded(g2)
        gram[n : n + C2, :] = g2[:, :n] + g2[:, n:]

        m = n // GROUPS
        for g in range(GROUPS):
            acc = jnp.zeros((2 * m, 2 * n), F32)
            for t in range(half):
                at = wland.at[t, pl.ds(g * m, m)]
                send(at, at, w_s.at[0], w_r.at[t * GROUPS + g], (2, me_r)).wait_recv()
                acc = acc + nt(stacked(wland[t, g * m : (g + 1) * m, :]), big[t])
            acc = folded(acc)
            gram[g * m : (g + 1) * m, :] = acc[:, :n] + acc[:, n:]

        y = folded(nn(stacked(gram[...]), pick))
        y0, y1 = y[:, :count], y[:, count:]

        def put(row, lo, hi, masks):
            a, b = y0[lo:hi], y1[lo:hi]
            m0, m1 = masks
            part[row : row + 1, :] = jnp.sum(
                jnp.where(m0, a, 0.0) - jnp.where(m1, b, 0.0), axis=0, keepdims=True
            )
            part[row + 1 : row + 2, :] = jnp.sum(
                jnp.where(m1, a, 0.0) + jnp.where(m0, b, 0.0), axis=0, keepdims=True
            )

        part[...] = jnp.zeros_like(part)
        put(0, n + C2, n + C2 + 8, [rows_of((8, count)) == c for c in range(2)])
        put(2, n, n + C2, [rows_of((C2, count)) == c * P_ + setting(2) for c in range(2)])
        put(4, 0, n, [rows_of((n, count)) == setting(2) * C2 + c * P_ + setting(3) for c in range(2)])
        fin[me_r] = part[...]
        for copy in finals(1, S - 1):
            copy.start()
        for t in range(half):
            x_copy(t).wait_send()

    def fin_wait(r):
        send(fin.at[r], fin.at[r], f_s.at[0], f_r.at[r], (1, (me_r + 1) % R)).wait_recv()

    @pl.when(me_s <= 1)
    def _():
        for d in range(1, R):
            fin_wait((me_r + d) % R)

    @pl.when(me_s > 1)
    def _():
        for r in range(R):
            fin_wait(r)

    value = fin[0]
    for r in range(1, R):
        value = value + fin[r]
    total[...] = value
    v = total[...]
    pair = jnp.where(me_s <= 1, v[0:2], jnp.where(me_s == 2, v[2:4], v[4:6]))
    for c in range(2):
        for m in range(micro):
            out_ref[0, c, m : m + 1, :] = pair[c : c + 1, m * batch : (m + 1) * batch]

    @pl.when(me_s != 1)
    def _():
        set_copy().wait_send()

    @pl.when(me_s == 0)
    def _():
        for d in range(R):
            to = (me_r + d) % R
            send(snd.at[to], uland.at[me_r], u_s.at[to], u_r.at[me_r], (1, to)).wait_send()
        for copy in finals(0, 1):
            copy.wait_send()

    @pl.when(me_s == 1)
    def _():
        for copy in finals(1, S - 1):
            copy.wait_send()

    @pl.when(me_s == 2)
    def _():
        for t in range(half):
            v2_copy(t).wait_send()
            for g in range(GROUPS):
                w_copy(g, t).wait_send()

    @pl.when(me_s == 3)
    def _():
        for d in range(R):
            to = (me_r + d) % R
            send(own, vland.at[me_r], v_s.at[d], v_r.at[me_r], (2, to)).wait_send()


def local(bitstrings, boundary, stem_tensor, probe_vectors, inbound_permutations):
    S, R = lax.axis_size("section"), lax.axis_size("stem")
    rows, settings, K = stem_tensor.shape[2:]
    micro, batch, qubits = bitstrings.shape[1:]
    count = micro * batch
    C2 = 2 * settings
    n = settings * C2
    half = R // 2
    dma = pltpu.SemaphoreType.DMA
    scratch = [
        pltpu.VMEM((SLOTS, K // LANES, 2, STEP * settings, LANES), F32),
        pltpu.VMEM((2, 2, settings, rows, K), BF16),
        pltpu.VMEM((K, K), BF16),
        pltpu.VMEM((C2, K), F32),
        pltpu.VMEM((C2, rows), F32),
        pltpu.VMEM((S, 8, count), F32),
        pltpu.VMEM((8, count), F32),
        pltpu.VMEM((R, C2, rows), F32),
        pltpu.VMEM((R, C2, rows), F32),
        pltpu.VMEM((R, C2, rows), F32),
        pltpu.VMEM((half, 2 * n, rows), BF16),
        pltpu.VMEM((2 * n, K), BF16),
        pltpu.VMEM((half, n, rows), F32),
        pltpu.VMEM((half, n, rows), F32),
        pltpu.VMEM((half, n, rows), F32),
        pltpu.VMEM((n, rows), F32),
        pltpu.VMEM((half, n, rows), F32),
        pltpu.VMEM((half, C2, rows), F32),
        pltpu.VMEM((n + C2 + 8, n), F32),
        pltpu.VMEM((8, count), F32),
        pltpu.VMEM((R, 8, count), F32),
        pltpu.VMEM((8, count), F32),
        dma((SLOTS,)),
        dma((1,)),
        dma((S,)),
        dma((R,)),
        dma((R,)),
        dma((R,)),
        dma((R,)),
        dma((half,)),
        dma((half,)),
        dma((half,)),
        dma((half,)),
        dma((GROUPS * half,)),
        dma((GROUPS * half,)),
        dma((S * R,)),
        dma((R,)),
    ]
    out = pl.pallas_call(
        functools.partial(kernel, S, R, rows, settings, K, count),
        out_shape=jax.ShapeDtypeStruct((1, 2, micro, batch), F32),
        in_specs=[VMEM, SMEM, SMEM, VMEM, VMEM, ANY],
        out_specs=VMEM,
        scratch_shapes=scratch,
        compiler_params=pltpu.CompilerParams(
            collective_id=1, has_side_effects=True, vmem_limit_bytes=67_000_000
        ),
    )(
        jnp.transpose(bitstrings[0], (2, 0, 1)),
        boundary,
        inbound_permutations,
        inbound_permutations,
        probe_vectors.reshape(2, K),
        stem_tensor.reshape(2, rows * settings, K),
    )
    return out


def solution(mesh):
    return jax.shard_map(
        local,
        mesh=mesh,
        in_specs=(
            P("section", None, None, None),
            P(),
            P("section", None, "stem", None, None),
            P("section", None, None),
            P(),
        ),
        out_specs=P("section", None, None, None),
        check_vma=False,
    )
```

```python
import functools

import jax
import jax.numpy as jnp
from jax import lax
from jax.experimental import pallas as pl
from jax.experimental.pallas import tpu as pltpu
from jax.sharding import PartitionSpec as P

MESH = pl.DeviceIdType.MESH
VMEM = pl.BlockSpec(memory_space=pltpu.VMEM)
ANY = pl.BlockSpec(memory_space=pl.ANY)
F32, BF16 = jnp.float32, jnp.bfloat16
LANES = 128
SLOTS = 4
STEP = 16
VIA = 3


def send(src, dst, send_sem, recv_sem, target):
    return pltpu.make_async_remote_copy(
        src_ref=src, dst_ref=dst, send_sem=send_sem, recv_sem=recv_sem, device_id=target, device_id_type=MESH
    )


def nn(a, b):
    return jnp.dot(a, b, preferred_element_type=F32)


def nt(a, b):
    return lax.dot_general(a, b, (((1,), (1,)), ((), ())), preferred_element_type=F32)


def halves(x):
    hi = x.astype(BF16)
    return hi, (x - hi.astype(F32)).astype(BF16)


def stacked(x):
    return jnp.concatenate(halves(x), axis=0)


def folded(y):
    n = y.shape[0] // 2
    return y[:n] + y[n:]


def turned(x):
    n = x.shape[0] // 2
    return jnp.concatenate([-x[n:], x[:n]], axis=0)


def rows_of(shape):
    return lax.broadcasted_iota(jnp.int32, shape, 0)


def lanes_of(shape):
    return lax.broadcasted_iota(jnp.int32, shape, 1)


def kernel(
    S, R, rows, P_, K, count,
    bits_hbm, bnd_hbm, perm_hbm, probe_hbm, stem_ref, out_ref,
    bits_ref, bnd_ref, perm0_ref, perm_ref, probe_ref,
    buf, hl, place, marks, masks, vecs, tails, wide, own, sets, set_own, uland, vland, snd, big, bighl, mine, other, xland, wown,
    wland, v2own, v2land, gram, part, fin,
    small_sem, load_sem, set_s, set_r, u_s, u_r, v_s, v_r, v2_s, v2_r, x_s, x_r, w_s, w_r, f_s, f_r,
):
    me_s, me_r = lax.axis_index("section"), lax.axis_index("stem")
    half = R // 2
    parity = me_r % 2
    partner = me_r + 1 - 2 * parity
    chunks = rows // STEP
    C2 = 2 * P_
    tiles = K // LANES

    def load(i):
        slot = i % SLOTS
        for j in range(tiles):
            pltpu.make_async_copy(
                stem_ref.at[:, pl.ds(i * STEP * P_, STEP * P_), pl.ds(j * LANES, LANES)],
                buf.at[slot, j],
                load_sem.at[slot],
            ).start()

    def loaded(slot):
        pltpu.make_async_copy(buf.at[slot], buf.at[slot], load_sem.at[slot]).wait()

    smalls = [
        pltpu.make_async_copy(src, dst, small_sem.at[e])
        for e, (src, dst) in enumerate(
            [(perm_hbm, perm_ref), (probe_hbm, probe_ref), (bits_hbm, bits_ref), (bnd_hbm, bnd_ref), (perm_hbm, perm0_ref)]
        )
    ]
    load(0)
    for copy in smalls:
        copy.start()
    for i in range(1, min(SLOTS, chunks)):
        load(i)

    barrier = pltpu.get_barrier_semaphore()
    for e in range(S):
        for d in range(R):
            if e + d:
                pl.semaphore_signal(
                    barrier, inc=1, device_id=((me_s + e) % S, (me_r + d) % R), device_id_type=MESH
                )

    own[...] = jnp.zeros_like(own)
    wide[...] = jnp.zeros_like(wide)
    for copy in smalls:
        copy.wait()

    qubits, micro, batch = bits_ref.shape
    codes = bits_ref[0].astype(F32)
    for q in range(1, qubits):
        codes = codes + float(2**q) * bits_ref[q].astype(F32)
    spread = jnp.zeros((8, count), F32)
    for m in range(micro):
        shift = (lanes_of((batch, count)) == rows_of((batch, count)) + m * batch).astype(F32).astype(BF16)
        spread = spread + nn(jnp.broadcast_to(codes[m : m + 1, :], (8, batch)).astype(BF16), shift)
    set_own[...] = spread

    blocks = tiles // chunks
    parts = 2 if rows % (2 * LANES) == 0 else 1

    def one(hit):
        return hit.astype(F32).astype(BF16)

    def columns(row):
        return jnp.broadcast_to(row, (LANES, LANES)).T

    @pl.when(me_s == 0)
    def _():
        row = perm_ref[1:2, :]
        place[0:LANES, :] = one(rows_of((LANES, K)) == row % LANES)
        marks[...] = jnp.broadcast_to(row // LANES, (2 * C2, K))

    @pl.when(me_s == 2)
    def _():
        row = perm_ref[3:4, :]
        high = jnp.broadcast_to(row // LANES, (2 * C2, K))
        for a in range(tiles):
            masks[a * 2 * C2 : (a + 1) * 2 * C2, :] = one(high == a)
        low = (row % LANES).astype(F32)
        for b in range(tiles):
            at = slice(b * LANES, (b + 1) * LANES)
            place[at, 0:LANES] = one(columns(low[:, at]) == lanes_of((LANES, LANES)).astype(F32))

    def build(i):
        for b in range(blocks):
            start = pl.multiple_of((i * blocks + b) * LANES, LANES)
            col = columns(perm_ref[2:3, pl.ds(start, LANES)].astype(F32))
            for j in range(tiles):
                target = (lanes_of((LANES, LANES)) + j * LANES).astype(F32)
                place[pl.ds(start, LANES), j * LANES : (j + 1) * LANES] = one(col == target)

    def first(i, slot):
        scal = []
        for k in range(STEP):
            at = perm0_ref[0, me_r * rows + i * STEP + k]
            scal.append((bnd_ref[0, at], bnd_ref[1, at]))
        span = 4
        for g in range(tiles // span):
            cols = [slice((g * span + t) * LANES, (g * span + t + 1) * LANES) for t in range(span)]
            a = [wide[0:P_, js] for js in cols]
            b = [wide[P_:C2, js] for js in cols]
            for k in range(STEP):
                br, bi = scal[k]
                for t in range(span):
                    tr = buf[slot, g * span + t, 0, k * P_ : (k + 1) * P_, :]
                    ti = buf[slot, g * span + t, 1, k * P_ : (k + 1) * P_, :]
                    a[t] = a[t] + (br * tr - bi * ti)
                    b[t] = b[t] + (br * ti + bi * tr)
            for t in range(span):
                wide[0:P_, cols[t]] = a[t]
                wide[P_:C2, cols[t]] = b[t]

    def against_probe(i, slot):
        width = min(rows, LANES)
        block = pl.multiple_of((i * STEP // width) * width, width)
        lane = lanes_of((P_, width))
        at = pl.ds(block, width) if rows > width else slice(None)
        a, b = own[0:P_, at], own[P_:C2, at]
        for k in range(STEP):
            ar = jnp.zeros((P_, LANES), F32)
            ai = jnp.zeros((P_, LANES), F32)
            for j in range(tiles):
                js = slice(j * LANES, (j + 1) * LANES)
                tr = buf[slot, j, 0, k * P_ : (k + 1) * P_, :]
                ti = buf[slot, j, 1, k * P_ : (k + 1) * P_, :]
                pr, pi = wide[0:P_, js], wide[P_:C2, js]
                ar = ar + (tr * pr - ti * pi)
                ai = ai + (tr * pi + ti * pr)
            hit = lane == (i * STEP + k - block)
            a = jnp.where(hit, jnp.sum(ar, axis=1, keepdims=True), a)
            b = jnp.where(hit, jnp.sum(ai, axis=1, keepdims=True), b)
        own[0:P_, at] = a
        own[P_:C2, at] = b

    def split(i, slot):
        at = pl.ds(pl.multiple_of(i * STEP, STEP), STEP)

        def column(j, carry):
            js = pl.ds(pl.multiple_of(j * LANES, LANES), LANES)
            for c in range(2):
                for p in range(P_):
                    hi, lo = halves(buf[slot, j, c, pl.ds(p, STEP, P_), :])
                    hl[c, 0, p, at, js] = hi
                    hl[c, 1, p, at, js] = lo
            return carry

        lax.fori_loop(0, tiles, column, 0)

    @pl.when(me_s == 3)
    def _():
        wide[0:P_, :] = jnp.broadcast_to(probe_ref[0:1, :], (P_, K))
        wide[P_:C2, :] = jnp.broadcast_to(probe_ref[1:2, :], (P_, K))

    def stream(i, carry):
        slot = i % SLOTS
        loaded(slot)

        @pl.when(me_s == 0)
        def _():
            first(i, slot)

        @pl.when(me_s == 1)
        def _():
            build(i)
            split(i, slot)

        @pl.when(me_s == 2)
        def _():
            split(i, slot)

        @pl.when(me_s == 3)
        def _():
            against_probe(i, slot)

        @pl.when(i + SLOTS < chunks)
        def _():
            load(i + SLOTS)

        return carry

    def v_copy(e, d):
        to = (me_r + d) % R
        n = rows // parts
        at = (slice(None), pl.ds(e * n, n))
        return send(own.at[at], vland.at[(me_r,) + at], v_s.at[e * R + d], v_r.at[me_r * parts + e], (2, to))

    for e in range(parts):
        lax.fori_loop(e * (chunks // parts), (e + 1) * (chunks // parts), stream, 0)
        if e == 0:
            pl.semaphore_wait(barrier, S * R - 1)

        @pl.when(me_s == 3)
        def _():
            for d in range(R):
                v_copy(e, d).start()

    def set_copy():
        return send(set_own, sets.at[me_s], set_s.at[0], set_r.at[me_s], (1, me_r))

    def set_wait(s):
        send(sets.at[s], sets.at[s], set_s.at[0], set_r.at[s], (0, me_r)).wait_recv()

    @pl.when(me_s != 1)
    def _():
        set_copy().start()

    def finals(section, lo):
        return [
            send(part, fin.at[me_r], f_s.at[e * R + d], f_r.at[me_r], (section + e, (me_r + d) % R))
            for e in range(lo)
            for d in range(R)
            if e + d
        ]

    setting = lambda s: sets[s, 0:1, :].astype(jnp.int32)

    @pl.when(me_s == 0)
    def _():
        u = stacked(wide[...])
        tall = jnp.concatenate([u[:, a * LANES : (a + 1) * LANES] for a in range(tiles)], axis=0)
        span = max(rows, LANES)

        def spot(d, carry):
            step = (me_r * rows // span + d) % (K // span)
            at = pl.ds(pl.multiple_of(step * span, span), span)
            z = nn(tails[...], place[0:LANES, at])
            mark = marks[:, at]
            got = z[0 : 2 * C2]
            for a in range(1, tiles):
                got = jnp.where(mark == a, z[a * 2 * C2 : (a + 1) * 2 * C2], got)
            got = folded(got)
            for e in range(span // rows):
                to = step * (span // rows) + e
                snd[to] = got[:, e * rows : (e + 1) * rows]
                send(snd.at[to], uland.at[me_r], u_s.at[to], u_r.at[me_r], (1, to)).start()
            return carry

        tails[...] = tall
        lax.fori_loop(0, K // span, spot, 0)
        ur, ui = wide[0:P_, :], wide[P_:C2, :]
        pr, pi = probe_ref[0:1, :], probe_ref[1:2, :]
        hit = rows_of((P_, count)) == set_own[0:1, :].astype(jnp.int32)
        re = jnp.sum(ur * pr - ui * pi, axis=1, keepdims=True)
        im = jnp.sum(ur * pi + ui * pr, axis=1, keepdims=True)
        part[...] = jnp.zeros_like(part)
        part[0:1, :] = jnp.sum(jnp.where(hit, re, 0.0), axis=0, keepdims=True)
        part[1:2, :] = jnp.sum(jnp.where(hit, im, 0.0), axis=0, keepdims=True)
        fin[me_r] = part[...]
        for copy in finals(0, 1):
            copy.start()

    def w_copy(p, t):
        to = (me_r + 2 * t) % R
        at = pl.ds(pl.multiple_of(p * C2, C2), C2)
        return send(
            wown.at[at], wland.at[me_r // 2, at], w_s.at[p * half + t], w_r.at[(me_r // 2) * P_ + p], (jnp.minimum(p // VIA, 1), to)
        )

    def relay(p, t):
        at = pl.ds(pl.multiple_of(p * C2, C2), C2)
        return send(wland.at[t, at], wland.at[t, at], w_s.at[p * half + t], w_r.at[t * P_ + p], (1, me_r))

    def w_wait(p, t):
        relay(p, t).wait_recv()

    def v2_copy(e, t):
        to = (me_r + 2 * t) % R
        at = pl.ds(pl.multiple_of(e * P_, P_), P_)
        return send(v2own.at[e], v2land.at[me_r // 2, at], v2_s.at[e * half + t], v2_r.at[(me_r // 2) * 2 + e], (1, to))

    @pl.when(me_s == 0)
    def _():
        def hop(q, carry):
            for t in range(half):
                w_wait(q, t)
                relay(q, t).start()
            return carry

        lax.fori_loop(0, VIA, hop, 0)

    @pl.when(me_s == 2)
    def _():
        for r in range(R):
            for e in range(parts):
                n = rows // parts
                at = vland.at[r, :, pl.ds(e * n, n)]
                send(at, at, v_s.at[0], v_r.at[r * parts + e], (3, me_r)).wait_recv()
        z = None
        for r in range(R):
            at = slice(r * rows, (r + 1) * rows)
            v = stacked(vland[r])
            tall = jnp.concatenate(
                [masks[a * 2 * C2 : (a + 1) * 2 * C2, at] * v for a in range(tiles)], axis=0
            )
            y = nn(tall, place[at, 0:LANES])
            z = y if z is None else z + y
        y = jnp.concatenate([z[a * 2 * C2 : (a + 1) * 2 * C2] for a in range(tiles)], axis=1)
        hi, lo = y[:C2], y[C2:]
        probe = probe_ref[...]

        def ends(x):
            return [h.astype(F32) for h in halves(jnp.concatenate([x] * (P_ // 2), axis=0))]

        straight = jnp.concatenate([hi, lo] + ends(probe), axis=0).astype(BF16)
        crossed = jnp.concatenate([turned(hi), turned(lo)] + ends(turned(probe)), axis=0).astype(BF16)
        vecs[0] = straight
        vecs[1] = crossed
        v2own[...] = jnp.zeros_like(v2own)

        def back(p, carry):
            z = nt(vecs[0], hl[0, 0, p]) + nt(vecs[1], hl[1, 0, p])
            z = z + nt(vecs[0], hl[0, 1, p]) + nt(vecs[1], hl[1, 1, p])
            wown[pl.ds(pl.multiple_of(p * C2, C2), C2), :] = folded(z[: 2 * C2])
            e = p // (P_ // 2)
            v2own[e] = jnp.where(rows_of((P_, rows)) // 2 == p % (P_ // 2), folded(z[2 * C2 :]), v2own[e])
            for t in range(half):
                w_copy(p, t).start()

            @pl.when((p + 1) % (P_ // 2) == 0)
            def _():
                for t in range(half):
                    v2_copy(e, t).start()

            return carry

        lax.fori_loop(0, P_, back, 0)

    @pl.when(me_s == 1)
    def _():
        for r in range(R):
            send(uland.at[r], uland.at[r], u_s.at[0], u_r.at[r], (0, me_r)).wait_recv()
        x = uland[0]
        for r in range(1, R):
            x = x + uland[r]
        straight, crossed = stacked(x), stacked(turned(x))

        def front(p, carry):
            z = nn(straight, hl[0, 0, p]) + nn(crossed, hl[1, 0, p])
            z = z + nn(straight, hl[0, 1, p]) + nn(crossed, hl[1, 1, p])
            hi, lo = halves(folded(z))
            at = pl.multiple_of(p * C2, C2)
            bighl[pl.ds(at, C2), :] = hi
            bighl[pl.ds(pl.multiple_of(P_ * C2 + p * C2, C2), C2), :] = lo
            return carry

        lax.fori_loop(0, P_, front, 0)
        n = P_ * C2

        def shuffled(q):
            return folded(nt(bighl[...], place[pl.ds(pl.multiple_of(q * rows, rows), rows), :]))

        def x_copy(t):
            return send(other.at[t], xland.at[t], x_s.at[t], x_r.at[t], (1, partner))

        def give(t, carry):
            other[t] = shuffled(2 * t + 1 - parity)
            x_copy(t).start()
            return carry

        def keep(t, carry):
            mine[t] = shuffled(2 * t + parity)
            return carry

        lax.fori_loop(0, half, give, 0)
        lax.fori_loop(0, half, keep, 0)
        probes = jnp.concatenate([probe_ref[...], jnp.zeros((6, K), F32)], axis=0)
        g1 = folded(nt(stacked(probes), bighl[...]))
        gram[n + C2 : n + C2 + 8, :] = g1[:, :n] + g1[:, n:]
        sets[1] = set_own[...]
        for s in (0, 2, 3):
            set_wait(s)
        hits = [rows_of((n, count)) == setting(1) * C2 + c * P_ + setting(0) for c in range(2)]
        pick = jnp.concatenate([h.astype(F32) for h in hits], axis=1).astype(BF16)

        for t in range(half):
            x_copy(t).wait_recv()
            hi, lo = halves(mine[t] + xland[t])
            big[t, 0:n, :] = hi
            big[t, n : 2 * n, :] = lo

        def inner(q, carry):
            p = q
            at = pl.ds(pl.multiple_of(p * C2, C2), C2)
            for t in range(half):
                w_wait(p, t)
            acc = nt(stacked(wland[0, at, :]), big[0])
            for t in range(1, half):
                acc = acc + nt(stacked(wland[t, at, :]), big[t])
            acc = folded(acc)
            gram[at, :] = acc[:, :n] + acc[:, n:]
            return carry

        lax.fori_loop(0, P_, inner, 0)
        acc = None
        for t in range(half):
            for e in range(2):
                at = v2land.at[t, pl.ds(e * P_, P_)]
                send(at, at, v2_s.at[0], v2_r.at[t * 2 + e], (2, me_r)).wait_recv()
            got = nt(stacked(v2land[t]), big[t])
            acc = got if acc is None else acc + got
        acc = folded(acc)
        gram[n : n + C2, :] = acc[:, :n] + acc[:, n:]

        y = folded(nn(stacked(gram[...]), pick))
        y0, y1 = y[:, :count], y[:, count:]

        def put(row, lo, hi, masks):
            a, b = y0[lo:hi], y1[lo:hi]
            m0, m1 = masks
            part[row : row + 1, :] = jnp.sum(
                jnp.where(m0, a, 0.0) - jnp.where(m1, b, 0.0), axis=0, keepdims=True
            )
            part[row + 1 : row + 2, :] = jnp.sum(
                jnp.where(m1, a, 0.0) + jnp.where(m0, b, 0.0), axis=0, keepdims=True
            )

        part[...] = jnp.zeros_like(part)
        put(0, n + C2, n + C2 + 8, [rows_of((8, count)) == c for c in range(2)])
        put(2, n, n + C2, [rows_of((C2, count)) == setting(2) * 2 + c for c in range(2)])
        put(4, 0, n, [rows_of((n, count)) == setting(2) * C2 + c * P_ + setting(3) for c in range(2)])
        fin[me_r] = part[...]
        for copy in finals(1, S - 1):
            copy.start()
        for t in range(half):
            x_copy(t).wait_send()

    def fin_wait(r):
        send(fin.at[r], fin.at[r], f_s.at[0], f_r.at[r], (1, (me_r + 1) % R)).wait_recv()

    @pl.when(me_s <= 1)
    def _():
        for d in range(1, R):
            fin_wait((me_r + d) % R)

    @pl.when(me_s > 1)
    def _():
        for r in range(R):
            fin_wait(r)

    value = fin[0]
    for r in range(1, R):
        value = value + fin[r]
    v = value
    pair = jnp.where(me_s <= 1, v[0:2], jnp.where(me_s == 2, v[2:4], v[4:6]))
    for c in range(2):
        for m in range(micro):
            out_ref[0, c, m : m + 1, :] = pair[c : c + 1, m * batch : (m + 1) * batch]

    @pl.when(me_s != 1)
    def _():
        set_copy().wait_send()

    @pl.when(me_s == 0)
    def _():
        for d in range(R):
            to = (me_r + d) % R
            send(snd.at[to], uland.at[me_r], u_s.at[to], u_r.at[me_r], (1, to)).wait_send()
        for copy in finals(0, 1):
            copy.wait_send()
        for p in range(VIA):
            for t in range(half):
                relay(p, t).wait_send()

    @pl.when(me_s == 1)
    def _():
        for copy in finals(1, S - 1):
            copy.wait_send()

    @pl.when(me_s == 2)
    def _():
        for t in range(half):
            for e in range(2):
                v2_copy(e, t).wait_send()
            for p in range(P_):
                w_copy(p, t).wait_send()

    @pl.when(me_s == 3)
    def _():
        for e in range(parts):
            for d in range(R):
                v_copy(e, d).wait_send()


def local(bitstrings, boundary, stem_tensor, probe_vectors, inbound_permutations):
    S, R = lax.axis_size("section"), lax.axis_size("stem")
    rows, settings, K = stem_tensor.shape[2:]
    micro, batch, qubits = bitstrings.shape[1:]
    count = micro * batch
    C2 = 2 * settings
    n = settings * C2
    half = R // 2
    dma = pltpu.SemaphoreType.DMA
    scratch = [
        pltpu.VMEM((qubits, micro, batch), jnp.int32),
        pltpu.SMEM(boundary.shape, F32),
        pltpu.SMEM(inbound_permutations.shape, jnp.int32),
        pltpu.VMEM(inbound_permutations.shape, jnp.int32),
        pltpu.VMEM((2, K), F32),
        pltpu.VMEM((SLOTS, K // LANES, 2, STEP * settings, LANES), F32),
        pltpu.VMEM((2, 2, settings, rows, K), BF16),
        pltpu.VMEM((K, K), BF16),
        pltpu.VMEM((2 * C2, K), jnp.int32),
        pltpu.VMEM((2 * C2 * (K // LANES), K), BF16),
        pltpu.VMEM((2, 3 * C2, K), BF16),
        pltpu.VMEM((2 * C2 * (K // LANES), LANES), BF16),
        pltpu.VMEM((C2, K), F32),
        pltpu.VMEM((C2, rows), F32),
        pltpu.VMEM((S, 8, count), F32),
        pltpu.VMEM((8, count), F32),
        pltpu.VMEM((R, C2, rows), F32),
        pltpu.VMEM((R, C2, rows), F32),
        pltpu.VMEM((R, C2, rows), F32),
        pltpu.VMEM((half, 2 * n, rows), BF16),
        pltpu.VMEM((2 * n, K), BF16),
        pltpu.VMEM((half, n, rows), F32),
        pltpu.VMEM((half, n, rows), F32),
        pltpu.VMEM((half, n, rows), F32),
        pltpu.VMEM((n, rows), F32),
        pltpu.VMEM((half, n, rows), F32),
        pltpu.VMEM((2, settings, rows), F32),
        pltpu.VMEM((half, C2, rows), F32),
        pltpu.VMEM((n + C2 + 8, n), F32),
        pltpu.VMEM((8, count), F32),
        pltpu.VMEM((R, 8, count), F32),
        dma((5,)),
        dma((SLOTS,)),
        dma((1,)),
        dma((S,)),
        dma((R,)),
        dma((R,)),
        dma((2 * R,)),
        dma((2 * R,)),
        dma((2 * half,)),
        dma((2 * half,)),
        dma((half,)),
        dma((half,)),
        dma((settings * half,)),
        dma((settings * half,)),
        dma((S * R,)),
        dma((R,)),
    ]
    out = pl.pallas_call(
        functools.partial(kernel, S, R, rows, settings, K, count),
        out_shape=jax.ShapeDtypeStruct((1, 2, micro, batch), F32),
        in_specs=[ANY] * 5,
        out_specs=VMEM,
        scratch_shapes=scratch,
        compiler_params=pltpu.CompilerParams(
            collective_id=1, has_side_effects=True, vmem_limit_bytes=67_000_000
        ),
    )(
        jnp.transpose(bitstrings[0], (2, 0, 1)),
        boundary,
        inbound_permutations,
        probe_vectors.reshape(2, K),
        stem_tensor.reshape(2, rows * settings, K),
    )
    return out


def solution(mesh):
    return jax.shard_map(
        local,
        mesh=mesh,
        in_specs=(
            P("section", None, None, None),
            P(),
            P("section", None, "stem", None, None),
            P("section", None, None),
            P(),
        ),
        out_specs=P("section", None, None, None),
        check_vma=False,
    )
```

```python
import functools

import jax
import jax.numpy as jnp
from jax import lax
from jax.experimental import pallas as pl
from jax.experimental.pallas import tpu as pltpu
from jax.sharding import PartitionSpec as P

MESH = pl.DeviceIdType.MESH
VMEM = pl.BlockSpec(memory_space=pltpu.VMEM)
ANY = pl.BlockSpec(memory_space=pl.ANY)
F32, BF16 = jnp.float32, jnp.bfloat16
LANES = 128
SLOTS = 4
STEP = 16
BLOCK = 256


def send(src, dst, send_sem, recv_sem, target):
    return pltpu.make_async_remote_copy(
        src_ref=src, dst_ref=dst, send_sem=send_sem, recv_sem=recv_sem, device_id=target, device_id_type=MESH
    )


def nn(a, b):
    return jnp.dot(a, b, preferred_element_type=F32)


def nt(a, b):
    return lax.dot_general(a, b, (((1,), (1,)), ((), ())), preferred_element_type=F32)


def halves(x):
    hi = x.astype(BF16)
    return hi, (x - hi.astype(F32)).astype(BF16)


def stacked(x):
    return jnp.concatenate(halves(x), axis=0)


def folded(y):
    n = y.shape[0] // 2
    return y[:n] + y[n:]


def turned(x):
    n = x.shape[0] // 2
    return jnp.concatenate([-x[n:], x[:n]], axis=0)


def rows_of(shape):
    return lax.broadcasted_iota(jnp.int32, shape, 0)


def lanes_of(shape):
    return lax.broadcasted_iota(jnp.int32, shape, 1)


def kernel(shared, S, R, rows, P_, K, count, *refs):
    refs = list(refs)
    if shared:
        refs.insert(13, refs[12])
    body(S, R, rows, P_, K, count, *refs)


def body(
    S, R, rows, P_, K, count,
    bits_hbm, bnd_hbm, perm_hbm, probe_hbm, stem_ref, out_ref,
    bits_ref, bnd_ref, perm0_ref, perm_ref, probe_ref,
    buf, hl, hlt, place, marks, masks, vecs, tails, wide, own, sets, set_own, uland, vland, snd, big, bighl, mine, other, xland, wown,
    wland, v2own, v2land, gram, part, fin,
    small_sem, load_sem, set_s, set_r, u_s, u_r, v_s, v_r, v2_s, v2_r, x_s, x_r, w_s, w_r, f_s, f_r,
):
    me_s, me_r = lax.axis_index("section"), lax.axis_index("stem")
    half = R // 2
    parity = me_r % 2
    partner = me_r + 1 - 2 * parity
    chunks = rows // STEP
    C2 = 2 * P_
    tiles = K // LANES

    block = min(rows, LANES)
    deep = block // STEP
    broad = tiles // deep
    across = tiles // broad
    turning = me_s == 2

    def load(i):
        slot = i % SLOTS
        for j in range(tiles):
            row = jnp.where(turning, (i // across) * deep + j // broad, i)
            col = jnp.where(turning, (i % across) * broad + j % broad, j)
            pltpu.make_async_copy(
                stem_ref.at[
                    :,
                    pl.ds(pl.multiple_of(row * STEP * P_, STEP * P_), STEP * P_),
                    pl.ds(pl.multiple_of(col * LANES, LANES), LANES),
                ],
                buf.at[slot, j],
                load_sem.at[slot],
            ).start()

    def loaded(slot):
        pltpu.make_async_copy(buf.at[slot], buf.at[slot], load_sem.at[slot]).wait()

    smalls = [
        pltpu.make_async_copy(src, dst, small_sem.at[e])
        for e, (src, dst) in enumerate(
            [(perm_hbm, perm_ref), (probe_hbm, probe_ref), (bits_hbm, bits_ref), (bnd_hbm, bnd_ref), (perm_hbm, perm0_ref)]
        )
    ]
    load(0)
    for copy in smalls:
        copy.start()
    for i in range(1, min(SLOTS, chunks)):
        load(i)

    barrier = pltpu.get_barrier_semaphore()
    for e in range(S):
        for d in range(R):
            if e + d:
                pl.semaphore_signal(
                    barrier, inc=1, device_id=((me_s + e) % S, (me_r + d) % R), device_id_type=MESH
                )

    own[...] = jnp.zeros_like(own)
    wide[...] = jnp.zeros_like(wide)
    for copy in smalls:
        copy.wait()

    qubits, micro, batch = bits_ref.shape
    codes = bits_ref[0].astype(F32)
    for q in range(1, qubits):
        codes = codes + float(2**q) * bits_ref[q].astype(F32)
    spread = jnp.zeros((8, count), F32)
    for m in range(micro):
        shift = (lanes_of((batch, count)) == rows_of((batch, count)) + m * batch).astype(F32).astype(BF16)
        spread = spread + nn(jnp.broadcast_to(codes[m : m + 1, :], (8, batch)).astype(BF16), shift)
    set_own[...] = spread

    blocks = tiles // chunks
    parts = 2 if rows % (2 * LANES) == 0 else 1

    def one(hit):
        return hit.astype(F32).astype(BF16)

    def columns(row):
        return jnp.broadcast_to(row, (LANES, LANES)).T

    @pl.when(me_s == 0)
    def _():
        row = perm_ref[1:2, :]
        place[0:LANES, :] = one(rows_of((LANES, K)) == row % LANES)
        marks[...] = jnp.broadcast_to(row // LANES, (2 * C2, K))

    @pl.when(me_s == 2)
    def _():
        row = perm_ref[3:4, :]
        high = jnp.broadcast_to(row // LANES, (2 * C2, K))
        for a in range(tiles):
            masks[a * 2 * C2 : (a + 1) * 2 * C2, :] = one(high == a)
        low = (row % LANES).astype(F32)
        for b in range(tiles):
            at = slice(b * LANES, (b + 1) * LANES)
            place[at, 0:LANES] = one(columns(low[:, at]) == lanes_of((LANES, LANES)).astype(F32))

    def build(i):
        for b in range(blocks):
            start = pl.multiple_of((i * blocks + b) * LANES, LANES)
            col = columns(perm_ref[2:3, pl.ds(start, LANES)].astype(F32))
            for j in range(tiles):
                target = (lanes_of((LANES, LANES)) + j * LANES).astype(F32)
                place[pl.ds(start, LANES), j * LANES : (j + 1) * LANES] = one(col == target)

    def first(i, slot):
        scal = []
        for k in range(STEP):
            at = perm0_ref[0, me_r * rows + i * STEP + k]
            scal.append((bnd_ref[0, at], bnd_ref[1, at]))
        span = 4
        for g in range(tiles // span):
            cols = [slice((g * span + t) * LANES, (g * span + t + 1) * LANES) for t in range(span)]
            a = [wide[0:P_, js] for js in cols]
            b = [wide[P_:C2, js] for js in cols]
            for k in range(STEP):
                br, bi = scal[k]
                for t in range(span):
                    tr = buf[slot, g * span + t, 0, k * P_ : (k + 1) * P_, :]
                    ti = buf[slot, g * span + t, 1, k * P_ : (k + 1) * P_, :]
                    a[t] = a[t] + (br * tr - bi * ti)
                    b[t] = b[t] + (br * ti + bi * tr)
            for t in range(span):
                wide[0:P_, cols[t]] = a[t]
                wide[P_:C2, cols[t]] = b[t]

    def against_probe(i, slot):
        width = min(rows, LANES)
        block = pl.multiple_of((i * STEP // width) * width, width)
        lane = lanes_of((P_, width))
        at = pl.ds(block, width) if rows > width else slice(None)
        a, b = own[0:P_, at], own[P_:C2, at]
        for k in range(STEP):
            ar = jnp.zeros((P_, LANES), F32)
            ai = jnp.zeros((P_, LANES), F32)
            for j in range(tiles):
                js = slice(j * LANES, (j + 1) * LANES)
                tr = buf[slot, j, 0, k * P_ : (k + 1) * P_, :]
                ti = buf[slot, j, 1, k * P_ : (k + 1) * P_, :]
                pr, pi = wide[0:P_, js], wide[P_:C2, js]
                ar = ar + (tr * pr - ti * pi)
                ai = ai + (tr * pi + ti * pr)
            hit = lane == (i * STEP + k - block)
            a = jnp.where(hit, jnp.sum(ar, axis=1, keepdims=True), a)
            b = jnp.where(hit, jnp.sum(ai, axis=1, keepdims=True), b)
        own[0:P_, at] = a
        own[P_:C2, at] = b

    def split(i, slot):
        at = pl.ds(pl.multiple_of(i * STEP, STEP), STEP)

        def column(j, carry):
            js = pl.ds(pl.multiple_of(j % (BLOCK // LANES) * LANES, LANES), LANES)
            for c in range(2):
                for p in range(P_):
                    hi, lo = halves(buf[slot, j, c, pl.ds(p, STEP, P_), :])
                    hl[c, 0, p, j // (BLOCK // LANES), at, js] = hi
                    hl[c, 1, p, j // (BLOCK // LANES), at, js] = lo
            return carry

        lax.fori_loop(0, tiles, column, 0)

    def split_turned(i, slot):
        at = pl.ds(pl.multiple_of(i // across * block, block), block) if rows > block else slice(None)

        def column(e, carry):
            j, c = e // 2, e % 2
            tile = (i % across) * broad + j
            js = pl.ds(pl.multiple_of(tile % (BLOCK // LANES) * LANES, LANES), LANES)
            for p in range(P_):
                x = [buf[slot, d * broad + j, c, pl.ds(p, STEP, P_), :] for d in range(deep)]
                hi, lo = halves(jnp.concatenate(x, axis=0).T)
                hlt[c, 0, p, tile // (BLOCK // LANES), js, at] = hi
                hlt[c, 1, p, tile // (BLOCK // LANES), js, at] = lo
            return carry

        lax.fori_loop(0, 2 * broad, column, 0)

    @pl.when(me_s == 3)
    def _():
        wide[0:P_, :] = jnp.broadcast_to(probe_ref[0:1, :], (P_, K))
        wide[P_:C2, :] = jnp.broadcast_to(probe_ref[1:2, :], (P_, K))

    def stream(i, carry):
        slot = i % SLOTS
        loaded(slot)

        @pl.when(me_s == 0)
        def _():
            first(i, slot)

        @pl.when(me_s == 1)
        def _():
            build(i)
            split(i, slot)

        @pl.when(me_s == 2)
        def _():
            split_turned(i, slot)

        @pl.when(me_s == 3)
        def _():
            against_probe(i, slot)

        @pl.when(i + SLOTS < chunks)
        def _():
            load(i + SLOTS)

        return carry

    def v_copy(e, d):
        to = (me_r + d) % R
        n = rows // parts
        at = (slice(None), pl.ds(e * n, n))
        return send(own.at[at], vland.at[(me_r,) + at], v_s.at[e * R + d], v_r.at[me_r * parts + e], (2, to))

    for e in range(parts):
        lax.fori_loop(e * (chunks // parts), (e + 1) * (chunks // parts), stream, 0)
        if e == 0:
            pl.semaphore_wait(barrier, S * R - 1)

        @pl.when(me_s == 3)
        def _():
            for d in range(R):
                v_copy(e, d).start()

    def set_copy():
        return send(set_own, sets.at[me_s], set_s.at[0], set_r.at[me_s], (1, me_r))

    def set_wait(s):
        send(sets.at[s], sets.at[s], set_s.at[0], set_r.at[s], (0, me_r)).wait_recv()

    @pl.when(me_s != 1)
    def _():
        set_copy().start()

    def finals(section, lo):
        return [
            send(part.at[e], fin.at[me_r], f_s.at[e * R + d], f_r.at[me_r], (section + e, (me_r + d) % R))
            for e in range(lo)
            for d in range(R)
            if e + d
        ]

    setting = lambda s: sets[s, 0:1, :].astype(jnp.int32)

    @pl.when(me_s == 0)
    def _():
        u = stacked(wide[...])
        tall = jnp.concatenate([u[:, a * LANES : (a + 1) * LANES] for a in range(tiles)], axis=0)
        span = max(rows, LANES)

        def spot(d, carry):
            step = (me_r * rows // span + d) % (K // span)
            at = pl.ds(pl.multiple_of(step * span, span), span)
            z = nn(tails[...], place[0:LANES, at])
            mark = marks[:, at]
            got = z[0 : 2 * C2]
            for a in range(1, tiles):
                got = jnp.where(mark == a, z[a * 2 * C2 : (a + 1) * 2 * C2], got)
            got = folded(got)
            for e in range(span // rows):
                to = step * (span // rows) + e
                snd[to] = got[:, e * rows : (e + 1) * rows]
                send(snd.at[to], uland.at[me_r], u_s.at[to], u_r.at[me_r], (1, to)).start()
            return carry

        tails[...] = tall
        lax.fori_loop(0, K // span, spot, 0)
        ur, ui = wide[0:P_, :], wide[P_:C2, :]
        pr, pi = probe_ref[0:1, :], probe_ref[1:2, :]
        hit = rows_of((P_, count)) == set_own[0:1, :].astype(jnp.int32)
        re = jnp.sum(ur * pr - ui * pi, axis=1, keepdims=True)
        im = jnp.sum(ur * pi + ui * pr, axis=1, keepdims=True)
        part[0, 0:1, :] = jnp.sum(jnp.where(hit, re, 0.0), axis=0, keepdims=True)
        part[0, 1:2, :] = jnp.sum(jnp.where(hit, im, 0.0), axis=0, keepdims=True)
        fin[me_r] = part[0]
        for copy in finals(0, 1):
            copy.start()

    mid = P_ // 2
    relayed = [q + q // (mid - 1) for q in range(mid)]
    spot = me_r // 2

    def w_rows(p):
        return pl.ds(pl.multiple_of(p * C2, C2), C2)

    def w_copy(p, t):
        at, to = w_rows(p), (me_r + 2 * t) % R
        return send(wown.at[at], wland.at[spot, at], w_s.at[p * half + t], w_r.at[spot * P_ + p], (1, to))

    def w_lend(p):
        at = w_rows(p)
        return send(wown.at[at], wland.at[spot, at], w_s.at[p * half], w_r.at[spot * P_ + p], (0, me_r))

    def relay(p, t):
        at, to = (spot, w_rows(p)), (me_r + 2 * t) % R
        return send(wland.at[at], wland.at[at], w_s.at[p * half + t], w_r.at[spot * P_ + p], (1, to))

    def w_wait(p, t):
        at = (t, w_rows(p))
        send(wland.at[at], wland.at[at], w_s.at[p * half], w_r.at[t * P_ + p], (2, me_r)).wait_recv()

    def v2_copy(e, t):
        to = (me_r + 2 * t) % R
        at = pl.ds(pl.multiple_of(e * P_, P_), P_)
        return send(v2own.at[e], v2land.at[me_r // 2, at], v2_s.at[e * half + t], v2_r.at[(me_r // 2) * 2 + e], (1, to))

    @pl.when(me_s == 0)
    def _():
        def hop(q, carry):
            p = q + q // (mid - 1)
            w_wait(p, spot)
            for t in range(half):
                relay(p, t).start()
            return carry

        lax.fori_loop(0, mid, hop, 0)

    @pl.when(me_s == 2)
    def _():
        for r in range(R):
            for e in range(parts):
                n = rows // parts
                at = vland.at[r, :, pl.ds(e * n, n)]
                send(at, at, v_s.at[0], v_r.at[r * parts + e], (3, me_r)).wait_recv()
        z = None
        for r in range(R):
            at = slice(r * rows, (r + 1) * rows)
            v = stacked(vland[r])
            tall = jnp.concatenate(
                [masks[a * 2 * C2 : (a + 1) * 2 * C2, at] * v for a in range(tiles)], axis=0
            )
            y = nn(tall, place[at, 0:LANES])
            z = y if z is None else z + y
        y = jnp.concatenate([z[a * 2 * C2 : (a + 1) * 2 * C2] for a in range(tiles)], axis=1)
        hi, lo = y[:C2], y[C2:]
        probe = probe_ref[...]

        def ends(x):
            return [h.astype(F32) for h in halves(jnp.concatenate([x] * (P_ // 2), axis=0))]

        straight = jnp.concatenate([hi, lo] + ends(probe), axis=0).astype(BF16)
        crossed = jnp.concatenate([turned(hi), turned(lo)] + ends(turned(probe)), axis=0).astype(BF16)
        vecs[0] = straight
        vecs[1] = crossed
        v2own[...] = jnp.zeros_like(v2own)

        def back(pair, carry):
            for odd in range(2):
                p = 2 * pair + odd
                z = None
                for c in range(2):
                    for h in range(2):
                        for b in range(K // BLOCK):
                            y = nn(vecs[c, :, b * BLOCK : (b + 1) * BLOCK], hlt[c, h, p, b])
                            z = y if z is None else z + y
                wown[pl.ds(pl.multiple_of(p * C2, C2), C2), :] = folded(z[: 2 * C2])
                e = p // (P_ // 2)
                v2own[e] = jnp.where(rows_of((P_, rows)) // 2 == p % (P_ // 2), folded(z[2 * C2 :]), v2own[e])

            @pl.when((pair + 1) % (P_ // 4) == 0)
            def _():
                for t in range(half):
                    v2_copy(pair // (P_ // 4), t).start()

            for odd in range(2):
                p = 2 * pair + odd
                lent = jnp.logical_or(p < mid - 1, p == mid)

                @pl.when(lent)
                def _():
                    w_lend(p).start()

                @pl.when(jnp.logical_not(lent))
                def _():
                    for t in range(half):
                        w_copy(p, t).start()

            return carry

        lax.fori_loop(0, P_ // 2, back, 0)

    @pl.when(me_s == 1)
    def _():
        for r in range(R):
            send(uland.at[r], uland.at[r], u_s.at[0], u_r.at[r], (0, me_r)).wait_recv()
        x = uland[0]
        for r in range(1, R):
            x = x + uland[r]
        straight, crossed = stacked(x), stacked(turned(x))

        def front(p, carry):
            for b in range(K // BLOCK):
                z = nn(straight, hl[0, 0, p, b]) + nn(crossed, hl[1, 0, p, b])
                z = z + nn(straight, hl[0, 1, p, b]) + nn(crossed, hl[1, 1, p, b])
                hi, lo = halves(folded(z))
                js = slice(b * BLOCK, (b + 1) * BLOCK)
                bighl[pl.ds(pl.multiple_of(p * C2, C2), C2), js] = hi
                bighl[pl.ds(pl.multiple_of(P_ * C2 + p * C2, C2), C2), js] = lo
            return carry

        lax.fori_loop(0, P_, front, 0)
        n = P_ * C2

        def shuffled(q):
            return folded(nt(bighl[...], place[pl.ds(pl.multiple_of(q * rows, rows), rows), :]))

        def x_copy(t):
            return send(other.at[t], xland.at[t], x_s.at[t], x_r.at[t], (1, partner))

        def give(t, carry):
            other[t] = shuffled(2 * t + 1 - parity)
            x_copy(t).start()
            return carry

        def keep(t, carry):
            mine[t] = shuffled(2 * t + parity)
            return carry

        lax.fori_loop(0, half, give, 0)
        lax.fori_loop(0, half, keep, 0)
        probes = jnp.concatenate([probe_ref[...], jnp.zeros((6, K), F32)], axis=0)
        g1 = folded(nt(stacked(probes), bighl[...]))
        gram[n + C2 : n + C2 + 8, :] = g1[:, :n] + g1[:, n:]
        sets[1] = set_own[...]
        for s in (0, 2, 3):
            set_wait(s)
        hits = [rows_of((n, count)) == setting(1) * C2 + c * P_ + setting(0) for c in range(2)]
        pick = jnp.concatenate([h.astype(F32) for h in hits], axis=1).astype(BF16)

        for t in range(half):
            x_copy(t).wait_recv()
            hi, lo = halves(mine[t] + xland[t])
            big[t, 0:n, :] = hi
            big[t, n : 2 * n, :] = lo

        def inner(q, carry):
            p = q + q // mid - mid * (q // (P_ - 1))
            at = pl.ds(pl.multiple_of(p * C2, C2), C2)
            for t in range(half):
                w_wait(p, t)
            acc = nt(stacked(wland[0, at, :]), big[0])
            for t in range(1, half):
                acc = acc + nt(stacked(wland[t, at, :]), big[t])
            acc = folded(acc)
            gram[at, :] = acc[:, :n] + acc[:, n:]
            return carry

        lax.fori_loop(0, P_ - 1, inner, 0)
        acc = None
        for t in range(half):
            for e in range(2):
                at = v2land.at[t, pl.ds(e * P_, P_)]
                send(at, at, v2_s.at[0], v2_r.at[t * 2 + e], (2, me_r)).wait_recv()
            got = nt(stacked(v2land[t]), big[t])
            acc = got if acc is None else acc + got
        acc = folded(acc)
        gram[n : n + C2, :] = acc[:, :n] + acc[:, n:]
        lax.fori_loop(P_ - 1, P_, inner, 0)

        y = folded(nn(stacked(gram[...]), pick))
        y0, y1 = y[:, :count], y[:, count:]

        def put(row, lo, hi, masks):
            a, b = y0[lo:hi], y1[lo:hi]
            m0, m1 = masks
            part[row, 0:1, :] = jnp.sum(
                jnp.where(m0, a, 0.0) - jnp.where(m1, b, 0.0), axis=0, keepdims=True
            )
            part[row, 1:2, :] = jnp.sum(
                jnp.where(m1, a, 0.0) + jnp.where(m0, b, 0.0), axis=0, keepdims=True
            )

        put(0, n + C2, n + C2 + 8, [rows_of((8, count)) == c for c in range(2)])
        put(1, n, n + C2, [rows_of((C2, count)) == setting(2) * 2 + c for c in range(2)])
        put(2, 0, n, [rows_of((n, count)) == setting(2) * C2 + c * P_ + setting(3) for c in range(2)])
        fin[me_r] = part[0]
        for copy in finals(1, S - 1):
            copy.start()
        for t in range(half):
            x_copy(t).wait_send()

    def fin_wait(r):
        send(fin.at[r], fin.at[r], f_s.at[0], f_r.at[r], (1, (me_r + 1) % R)).wait_recv()

    @pl.when(me_s <= 1)
    def _():
        for d in range(1, R):
            fin_wait((me_r + d) % R)

    @pl.when(me_s > 1)
    def _():
        for r in range(R):
            fin_wait(r)

    value = fin[0]
    for r in range(1, R):
        value = value + fin[r]
    for c in range(2):
        for m in range(micro):
            out_ref[0, c, m : m + 1, :] = value[c : c + 1, m * batch : (m + 1) * batch]

    @pl.when(me_s != 1)
    def _():
        set_copy().wait_send()

    @pl.when(me_s == 0)
    def _():
        for d in range(R):
            to = (me_r + d) % R
            send(snd.at[to], uland.at[me_r], u_s.at[to], u_r.at[me_r], (1, to)).wait_send()
        for copy in finals(0, 1):
            copy.wait_send()
        for p in relayed:
            for t in range(half):
                relay(p, t).wait_send()

    @pl.when(me_s == 1)
    def _():
        for copy in finals(1, S - 1):
            copy.wait_send()

    @pl.when(me_s == 2)
    def _():
        for t in range(half):
            for e in range(2):
                v2_copy(e, t).wait_send()
            for p in range(P_):
                if p not in relayed:
                    w_copy(p, t).wait_send()
        for p in relayed:
            w_lend(p).wait_send()

    @pl.when(me_s == 3)
    def _():
        for e in range(parts):
            for d in range(R):
                v_copy(e, d).wait_send()


def local(bitstrings, boundary, stem_tensor, probe_vectors, inbound_permutations):
    S, R = lax.axis_size("section"), lax.axis_size("stem")
    rows, settings, K = stem_tensor.shape[2:]
    micro, batch, qubits = bitstrings.shape[1:]
    count = micro * batch
    C2 = 2 * settings
    n = settings * C2
    half = R // 2
    dma = pltpu.SemaphoreType.DMA
    scratch = [
        pltpu.VMEM((qubits, micro, batch), jnp.int32),
        pltpu.SMEM(boundary.shape, F32),
        pltpu.SMEM(inbound_permutations.shape, jnp.int32),
        pltpu.VMEM(inbound_permutations.shape, jnp.int32),
        pltpu.VMEM((2, K), F32),
        pltpu.VMEM((SLOTS, K // LANES, 2, STEP * settings, LANES), F32),
        pltpu.VMEM((2, 2, settings, K // BLOCK, rows, BLOCK), BF16),
        pltpu.VMEM((2, 2, settings, K // BLOCK, BLOCK, rows), BF16),
        pltpu.VMEM((K, K), BF16),
        pltpu.VMEM((2 * C2, K), jnp.int32),
        pltpu.VMEM((2 * C2 * (K // LANES), K), BF16),
        pltpu.VMEM((2, 3 * C2, K), BF16),
        pltpu.VMEM((2 * C2 * (K // LANES), LANES), BF16),
        pltpu.VMEM((C2, K), F32),
        pltpu.VMEM((C2, rows), F32),
        pltpu.VMEM((S, 8, count), F32),
        pltpu.VMEM((8, count), F32),
        pltpu.VMEM((R, C2, rows), F32),
        pltpu.VMEM((R, C2, rows), F32),
        pltpu.VMEM((R, C2, rows), F32),
        pltpu.VMEM((half, 2 * n, rows), BF16),
        pltpu.VMEM((2 * n, K), BF16),
        pltpu.VMEM((half, n, rows), F32),
        pltpu.VMEM((half, n, rows), F32),
        pltpu.VMEM((half, n, rows), F32),
        pltpu.VMEM((n, rows), F32),
        pltpu.VMEM((half, n, rows), F32),
        pltpu.VMEM((2, settings, rows), F32),
        pltpu.VMEM((half, C2, rows), F32),
        pltpu.VMEM((n + C2 + 8, n), F32),
        pltpu.VMEM((S - 1, 2, count), F32),
        pltpu.VMEM((R, 2, count), F32),
        dma((5,)),
        dma((SLOTS,)),
        dma((1,)),
        dma((S,)),
        dma((R,)),
        dma((R,)),
        dma((2 * R,)),
        dma((2 * R,)),
        dma((2 * half,)),
        dma((2 * half,)),
        dma((half,)),
        dma((half,)),
        dma((settings * half,)),
        dma((settings * half,)),
        dma((S * R,)),
        dma((R,)),
    ]
    shared = rows == BLOCK
    if shared:
        scratch.pop(7)
    out = pl.pallas_call(
        functools.partial(kernel, shared, S, R, rows, settings, K, count),
        out_shape=jax.ShapeDtypeStruct((1, 2, micro, batch), F32),
        in_specs=[ANY] * 5,
        out_specs=VMEM,
        scratch_shapes=scratch,
        compiler_params=pltpu.CompilerParams(
            collective_id=1, has_side_effects=True, vmem_limit_bytes=67_000_000
        ),
    )(
        jnp.transpose(bitstrings[0], (2, 0, 1)),
        boundary,
        inbound_permutations,
        probe_vectors.reshape(2, K),
        stem_tensor.reshape(2, rows * settings, K),
    )
    return out


def solution(mesh):
    return jax.shard_map(
        local,
        mesh=mesh,
        in_specs=(
            P("section", None, None, None),
            P(),
            P("section", None, "stem", None, None),
            P("section", None, None),
            P(),
        ),
        out_specs=P("section", None, None, None),
        check_vma=False,
    )
```

```python
import functools

import jax
import jax.numpy as jnp
from jax import lax
from jax.experimental import pallas as pl
from jax.experimental.pallas import tpu as pltpu
from jax.sharding import PartitionSpec as P

MESH = pl.DeviceIdType.MESH
VMEM = pl.BlockSpec(memory_space=pltpu.VMEM)
ANY = pl.BlockSpec(memory_space=pl.ANY)
F32, BF16 = jnp.float32, jnp.bfloat16
LANES = 128
SLOTS = 4
STEP = 16
BLOCK = 256


def send(src, dst, send_sem, recv_sem, target):
    return pltpu.make_async_remote_copy(
        src_ref=src, dst_ref=dst, send_sem=send_sem, recv_sem=recv_sem, device_id=target, device_id_type=MESH
    )


def nn(a, b):
    return jnp.dot(a, b, preferred_element_type=F32)


def nt(a, b):
    return lax.dot_general(a, b, (((1,), (1,)), ((), ())), preferred_element_type=F32)


def halves(x):
    hi = x.astype(BF16)
    return hi, (x - hi.astype(F32)).astype(BF16)


def stacked(x):
    return jnp.concatenate(halves(x), axis=0)


def folded(y):
    n = y.shape[0] // 2
    return y[:n] + y[n:]


def turned(x):
    n = x.shape[0] // 2
    return jnp.concatenate([-x[n:], x[:n]], axis=0)


def rows_of(shape):
    return lax.broadcasted_iota(jnp.int32, shape, 0)


def lanes_of(shape):
    return lax.broadcasted_iota(jnp.int32, shape, 1)


def kernel(shared, S, R, rows, P_, K, count, *refs):
    refs = list(refs)
    if shared:
        refs.insert(13, refs[12])
    body(S, R, rows, P_, K, count, *refs)


def body(
    S, R, rows, P_, K, count,
    bits_hbm, bnd_hbm, perm_hbm, probe_hbm, stem_ref, out_ref,
    bits_ref, bnd_ref, perm0_ref, perm_ref, probe_ref,
    buf, hl, hlt, place, marks, masks, vecs, tails, wide, own, sets, set_own, uland, vland, snd, big, bighl, mine, other, xland, wown,
    wland, v2own, v2land, gram, part, fin,
    small_sem, load_sem, set_s, set_r, u_s, u_r, v_s, v_r, v2_s, v2_r, x_s, x_r, w_s, w_r, f_s, f_r,
):
    me_s, me_r = lax.axis_index("section"), lax.axis_index("stem")
    half = R // 2
    parity = me_r % 2
    partner = me_r + 1 - 2 * parity
    chunks = rows // STEP
    C2 = 2 * P_
    tiles = K // LANES

    block = min(rows, LANES)
    deep = block // STEP
    broad = tiles // deep
    across = tiles // broad
    turning = me_s == 2

    def load(i):
        slot = i % SLOTS
        for j in range(tiles):
            row = jnp.where(turning, (i // across) * deep + j // broad, i)
            col = jnp.where(turning, (i % across) * broad + j % broad, j)
            pltpu.make_async_copy(
                stem_ref.at[
                    :,
                    pl.ds(pl.multiple_of(row * STEP * P_, STEP * P_), STEP * P_),
                    pl.ds(pl.multiple_of(col * LANES, LANES), LANES),
                ],
                buf.at[slot, j],
                load_sem.at[slot],
            ).start()

    def loaded(slot):
        pltpu.make_async_copy(buf.at[slot], buf.at[slot], load_sem.at[slot]).wait()

    smalls = [
        pltpu.make_async_copy(src, dst, small_sem.at[e])
        for e, (src, dst) in enumerate(
            [(perm_hbm, perm_ref), (probe_hbm, probe_ref), (bits_hbm, bits_ref), (bnd_hbm, bnd_ref), (perm_hbm, perm0_ref)]
        )
    ]
    load(0)
    for copy in smalls:
        copy.start()
    for i in range(1, min(SLOTS, chunks)):
        load(i)

    barrier = pltpu.get_barrier_semaphore()
    for e in range(S):
        for d in range(R):
            if e + d:
                pl.semaphore_signal(
                    barrier, inc=1, device_id=((me_s + e) % S, (me_r + d) % R), device_id_type=MESH
                )

    own[...] = jnp.zeros_like(own)
    wide[...] = jnp.zeros_like(wide)
    for copy in smalls:
        copy.wait()

    qubits, micro, batch = bits_ref.shape
    codes = bits_ref[0].astype(F32)
    for q in range(1, qubits):
        codes = codes + float(2**q) * bits_ref[q].astype(F32)
    spread = jnp.zeros((8, count), F32)
    for m in range(micro):
        shift = (lanes_of((batch, count)) == rows_of((batch, count)) + m * batch).astype(F32).astype(BF16)
        spread = spread + nn(jnp.broadcast_to(codes[m : m + 1, :], (8, batch)).astype(BF16), shift)
    set_own[...] = spread

    blocks = tiles // chunks
    parts = 2 if rows % (2 * LANES) == 0 else 1

    def one(hit):
        return hit.astype(F32).astype(BF16)

    def columns(row):
        return jnp.broadcast_to(row, (LANES, LANES)).T

    @pl.when(me_s == 0)
    def _():
        row = perm_ref[1:2, :]
        place[0:LANES, :] = one(rows_of((LANES, K)) == row % LANES)
        marks[...] = jnp.broadcast_to(row // LANES, (2 * C2, K))

    @pl.when(me_s == 2)
    def _():
        row = perm_ref[3:4, :]
        high = jnp.broadcast_to(row // LANES, (2 * C2, K))
        for a in range(tiles):
            masks[a * 2 * C2 : (a + 1) * 2 * C2, :] = one(high == a)
        low = (row % LANES).astype(F32)
        for b in range(tiles):
            at = slice(b * LANES, (b + 1) * LANES)
            place[at, 0:LANES] = one(columns(low[:, at]) == lanes_of((LANES, LANES)).astype(F32))

    def build(i):
        for b in range(blocks):
            start = pl.multiple_of((i * blocks + b) * LANES, LANES)
            col = columns(perm_ref[2:3, pl.ds(start, LANES)].astype(F32))
            for j in range(tiles):
                target = (lanes_of((LANES, LANES)) + j * LANES).astype(F32)
                place[pl.ds(start, LANES), j * LANES : (j + 1) * LANES] = one(col == target)

    def first(i, slot):
        scal = []
        for k in range(STEP):
            at = perm0_ref[0, me_r * rows + i * STEP + k]
            scal.append((bnd_ref[0, at], bnd_ref[1, at]))
        span = 4
        for g in range(tiles // span):
            cols = [slice((g * span + t) * LANES, (g * span + t + 1) * LANES) for t in range(span)]
            a = [wide[0:P_, js] for js in cols]
            b = [wide[P_:C2, js] for js in cols]
            for k in range(STEP):
                br, bi = scal[k]
                for t in range(span):
                    tr = buf[slot, g * span + t, 0, k * P_ : (k + 1) * P_, :]
                    ti = buf[slot, g * span + t, 1, k * P_ : (k + 1) * P_, :]
                    a[t] = a[t] + (br * tr - bi * ti)
                    b[t] = b[t] + (br * ti + bi * tr)
            for t in range(span):
                wide[0:P_, cols[t]] = a[t]
                wide[P_:C2, cols[t]] = b[t]

    def against_probe(i, slot):
        width = min(rows, LANES)
        block = pl.multiple_of((i * STEP // width) * width, width)
        lane = lanes_of((P_, width))
        at = pl.ds(block, width) if rows > width else slice(None)
        a, b = own[0:P_, at], own[P_:C2, at]
        for k in range(STEP):
            ar = jnp.zeros((P_, LANES), F32)
            ai = jnp.zeros((P_, LANES), F32)
            for j in range(tiles):
                js = slice(j * LANES, (j + 1) * LANES)
                tr = buf[slot, j, 0, k * P_ : (k + 1) * P_, :]
                ti = buf[slot, j, 1, k * P_ : (k + 1) * P_, :]
                pr, pi = wide[0:P_, js], wide[P_:C2, js]
                ar = ar + (tr * pr - ti * pi)
                ai = ai + (tr * pi + ti * pr)
            hit = lane == (i * STEP + k - block)
            a = jnp.where(hit, jnp.sum(ar, axis=1, keepdims=True), a)
            b = jnp.where(hit, jnp.sum(ai, axis=1, keepdims=True), b)
        own[0:P_, at] = a
        own[P_:C2, at] = b

    def split(i, slot):
        at = pl.ds(pl.multiple_of(i * STEP, STEP), STEP)

        def column(j, carry):
            js = pl.ds(pl.multiple_of(j % (BLOCK // LANES) * LANES, LANES), LANES)
            for c in range(2):
                for p in range(P_):
                    hi, lo = halves(buf[slot, j, c, pl.ds(p, STEP, P_), :])
                    hl[c, 0, p, j // (BLOCK // LANES), at, js] = hi
                    hl[c, 1, p, j // (BLOCK // LANES), at, js] = lo
            return carry

        lax.fori_loop(0, tiles, column, 0)

    def split_turned(i, slot):
        at = pl.ds(pl.multiple_of(i // across * block, block), block) if rows > block else slice(None)

        def column(e, carry):
            j, c = e // 2, e % 2
            tile = (i % across) * broad + j
            js = pl.ds(pl.multiple_of(tile % (BLOCK // LANES) * LANES, LANES), LANES)
            for p in range(P_):
                x = [buf[slot, d * broad + j, c, pl.ds(p, STEP, P_), :] for d in range(deep)]
                hi, lo = halves(jnp.concatenate(x, axis=0).T)
                hlt[c, 0, p, tile // (BLOCK // LANES), js, at] = hi
                hlt[c, 1, p, tile // (BLOCK // LANES), js, at] = lo
            return carry

        lax.fori_loop(0, 2 * broad, column, 0)

    @pl.when(me_s == 3)
    def _():
        wide[0:P_, :] = jnp.broadcast_to(probe_ref[0:1, :], (P_, K))
        wide[P_:C2, :] = jnp.broadcast_to(probe_ref[1:2, :], (P_, K))

    def stream(i, carry):
        slot = i % SLOTS
        loaded(slot)

        @pl.when(me_s == 0)
        def _():
            first(i, slot)

        @pl.when(me_s == 1)
        def _():
            build(i)
            split(i, slot)

        @pl.when(me_s == 2)
        def _():
            split_turned(i, slot)

        @pl.when(me_s == 3)
        def _():
            against_probe(i, slot)

        @pl.when(i + SLOTS < chunks)
        def _():
            load(i + SLOTS)

        return carry

    def v_copy(e, d):
        to = (me_r + d) % R
        n = rows // parts
        at = (slice(None), pl.ds(e * n, n))
        return send(own.at[at], vland.at[(me_r,) + at], v_s.at[e * R + d], v_r.at[me_r * parts + e], (2, to))

    for e in range(parts):
        lax.fori_loop(e * (chunks // parts), (e + 1) * (chunks // parts), stream, 0)
        if e == 0:
            pl.semaphore_wait(barrier, S * R - 1)

        @pl.when(me_s == 3)
        def _():
            for d in range(R):
                v_copy(e, d).start()

    def set_copy():
        return send(set_own, sets.at[me_s], set_s.at[0], set_r.at[me_s], (1, me_r))

    def set_wait(s):
        send(sets.at[s], sets.at[s], set_s.at[0], set_r.at[s], (0, me_r)).wait_recv()

    @pl.when(me_s != 1)
    def _():
        set_copy().start()

    def finals(section, lo):
        return [
            send(part.at[e], fin.at[me_r], f_s.at[e * R + d], f_r.at[me_r], (section + e, (me_r + d) % R))
            for e in range(lo)
            for d in range(R)
            if e + d
        ]

    setting = lambda s: sets[s, 0:1, :].astype(jnp.int32)

    @pl.when(me_s == 0)
    def _():
        u = stacked(wide[...])
        tall = jnp.concatenate([u[:, a * LANES : (a + 1) * LANES] for a in range(tiles)], axis=0)
        span = max(rows, LANES)

        def spot(d, carry):
            step = (me_r * rows // span + d) % (K // span)
            at = pl.ds(pl.multiple_of(step * span, span), span)
            z = nn(tails[...], place[0:LANES, at])
            mark = marks[:, at]
            got = z[0 : 2 * C2]
            for a in range(1, tiles):
                got = jnp.where(mark == a, z[a * 2 * C2 : (a + 1) * 2 * C2], got)
            got = folded(got)
            for e in range(span // rows):
                to = step * (span // rows) + e
                snd[to] = got[:, e * rows : (e + 1) * rows]
                send(snd.at[to], uland.at[me_r], u_s.at[to], u_r.at[me_r], (1, to)).start()
            return carry

        tails[...] = tall
        lax.fori_loop(0, K // span, spot, 0)
        ur, ui = wide[0:P_, :], wide[P_:C2, :]
        pr, pi = probe_ref[0:1, :], probe_ref[1:2, :]
        hit = rows_of((P_, count)) == set_own[0:1, :].astype(jnp.int32)
        re = jnp.sum(ur * pr - ui * pi, axis=1, keepdims=True)
        im = jnp.sum(ur * pi + ui * pr, axis=1, keepdims=True)
        part[0, 0:1, :] = jnp.sum(jnp.where(hit, re, 0.0), axis=0, keepdims=True)
        part[0, 1:2, :] = jnp.sum(jnp.where(hit, im, 0.0), axis=0, keepdims=True)
        fin[me_r] = part[0]
        for copy in finals(0, 1):
            copy.start()

    mid = P_ // 2
    relayed = [q + q // (mid - 1) for q in range(mid)]
    spot = me_r // 2

    def w_rows(p):
        return pl.ds(pl.multiple_of(p * C2, C2), C2)

    def w_copy(p, t):
        at, to = w_rows(p), (me_r + 2 * t) % R
        return send(wown.at[at], wland.at[spot, at], w_s.at[p * half + t], w_r.at[spot * P_ + p], (1, to))

    def w_lend(p):
        at = w_rows(p)
        return send(wown.at[at], wland.at[spot, at], w_s.at[p * half], w_r.at[spot * P_ + p], (0, me_r))

    def relay(p, t):
        at, to = (spot, w_rows(p)), (me_r + 2 * t) % R
        return send(wland.at[at], wland.at[at], w_s.at[p * half + t], w_r.at[spot * P_ + p], (1, to))

    def w_wait(p, t):
        at = (t, w_rows(p))
        send(wland.at[at], wland.at[at], w_s.at[p * half], w_r.at[t * P_ + p], (2, me_r)).wait_recv()

    def v2_copy(e, t):
        to = (me_r + 2 * t) % R
        at = pl.ds(pl.multiple_of(e * P_, P_), P_)
        return send(v2own.at[e], v2land.at[me_r // 2, at], v2_s.at[e * half + t], v2_r.at[(me_r // 2) * 2 + e], (1, to))

    @pl.when(me_s == 0)
    def _():
        def hop(q, carry):
            p = q + q // (mid - 1)
            w_wait(p, spot)
            for t in range(half):
                relay(p, t).start()
            return carry

        lax.fori_loop(0, mid, hop, 0)

    @pl.when(me_s == 2)
    def _():
        for r in range(R):
            for e in range(parts):
                n = rows // parts
                at = vland.at[r, :, pl.ds(e * n, n)]
                send(at, at, v_s.at[0], v_r.at[r * parts + e], (3, me_r)).wait_recv()
        z = None
        for r in range(R):
            at = slice(r * rows, (r + 1) * rows)
            v = stacked(vland[r])
            tall = jnp.concatenate(
                [masks[a * 2 * C2 : (a + 1) * 2 * C2, at] * v for a in range(tiles)], axis=0
            )
            y = nn(tall, place[at, 0:LANES])
            z = y if z is None else z + y
        y = jnp.concatenate([z[a * 2 * C2 : (a + 1) * 2 * C2] for a in range(tiles)], axis=1)
        hi, lo = y[:C2], y[C2:]
        probe = probe_ref[...]

        def ends(x):
            return [h.astype(F32) for h in halves(jnp.concatenate([x] * (P_ // 2), axis=0))]

        straight = jnp.concatenate([hi, lo] + ends(probe), axis=0).astype(BF16)
        crossed = jnp.concatenate([turned(hi), turned(lo)] + ends(turned(probe)), axis=0).astype(BF16)
        vecs[0] = straight
        vecs[1] = crossed
        v2own[...] = jnp.zeros_like(v2own)

        def back(pair, carry):
            for odd in range(2):
                p = 2 * pair + odd
                z = None
                for c in range(2):
                    for h in range(2):
                        for b in range(K // BLOCK):
                            y = nn(vecs[c, :, b * BLOCK : (b + 1) * BLOCK], hlt[c, h, p, b])
                            z = y if z is None else z + y
                wown[pl.ds(pl.multiple_of(p * C2, C2), C2), :] = folded(z[: 2 * C2])
                e = p // (P_ // 2)
                v2own[e] = jnp.where(rows_of((P_, rows)) // 2 == p % (P_ // 2), folded(z[2 * C2 :]), v2own[e])

            @pl.when((pair + 1) % (P_ // 4) == 0)
            def _():
                for t in range(half):
                    v2_copy(pair // (P_ // 4), t).start()

            for odd in range(2):
                p = 2 * pair + odd
                lent = jnp.logical_or(p < mid - 1, p == mid)

                @pl.when(lent)
                def _():
                    w_lend(p).start()

                @pl.when(jnp.logical_not(lent))
                def _():
                    for t in range(half):
                        w_copy(p, t).start()

            return carry

        lax.fori_loop(0, P_ // 2, back, 0)

    @pl.when(me_s == 1)
    def _():
        for r in range(R):
            send(uland.at[r], uland.at[r], u_s.at[0], u_r.at[r], (0, me_r)).wait_recv()
        x = uland[0]
        for r in range(1, R):
            x = x + uland[r]
        straight, crossed = stacked(x), stacked(turned(x))

        def front(p, carry):
            for b in range(K // BLOCK):
                z = nn(straight, hl[0, 0, p, b]) + nn(crossed, hl[1, 0, p, b])
                z = z + nn(straight, hl[0, 1, p, b]) + nn(crossed, hl[1, 1, p, b])
                hi, lo = halves(folded(z))
                js = slice(b * BLOCK, (b + 1) * BLOCK)
                bighl[pl.ds(pl.multiple_of(p * C2, C2), C2), js] = hi
                bighl[pl.ds(pl.multiple_of(P_ * C2 + p * C2, C2), C2), js] = lo
            return carry

        lax.fori_loop(0, P_, front, 0)
        n = P_ * C2

        def shuffled(q):
            return folded(nt(bighl[...], place[pl.ds(pl.multiple_of(q * rows, rows), rows), :]))

        def x_copy(t):
            return send(other.at[t], xland.at[t], x_s.at[t], x_r.at[t], (1, partner))

        def give(t, carry):
            other[t] = shuffled(2 * t + 1 - parity)
            x_copy(t).start()
            return carry

        def keep(t, carry):
            mine[t] = shuffled(2 * t + parity)
            return carry

        lax.fori_loop(0, half, give, 0)
        lax.fori_loop(0, half, keep, 0)
        probes = jnp.concatenate([probe_ref[...], jnp.zeros((6, K), F32)], axis=0)
        g1 = folded(nt(stacked(probes), bighl[...]))
        gram[n + C2 : n + C2 + 8, :] = g1[:, :n] + g1[:, n:]
        sets[1] = set_own[...]
        for s in (0, 2, 3):
            set_wait(s)
        hits = [rows_of((n, count)) == setting(1) * C2 + c * P_ + setting(0) for c in range(2)]
        pick = jnp.concatenate([h.astype(F32) for h in hits], axis=1).astype(BF16)

        for t in range(half):
            x_copy(t).wait_recv()
            hi, lo = halves(mine[t] + xland[t])
            big[t, 0:n, :] = hi
            big[t, n : 2 * n, :] = lo

        def inner(q, carry):
            p = q
            at = pl.ds(pl.multiple_of(p * C2, C2), C2)
            for t in range(half):
                w_wait(p, t)
            acc = nt(stacked(wland[0, at, :]), big[0])
            for t in range(1, half):
                acc = acc + nt(stacked(wland[t, at, :]), big[t])
            acc = folded(acc)
            gram[at, :] = acc[:, :n] + acc[:, n:]
            return carry

        lax.fori_loop(0, P_ - 1, inner, 0)
        acc = None
        for t in range(half):
            for e in range(2):
                at = v2land.at[t, pl.ds(e * P_, P_)]
                send(at, at, v2_s.at[0], v2_r.at[t * 2 + e], (2, me_r)).wait_recv()
            got = nt(stacked(v2land[t]), big[t])
            acc = got if acc is None else acc + got
        acc = folded(acc)
        gram[n : n + C2, :] = acc[:, :n] + acc[:, n:]
        lax.fori_loop(P_ - 1, P_, inner, 0)

        y = folded(nn(stacked(gram[...]), pick))
        y0, y1 = y[:, :count], y[:, count:]

        def put(row, lo, hi, masks):
            a, b = y0[lo:hi], y1[lo:hi]
            m0, m1 = masks
            part[row, 0:1, :] = jnp.sum(
                jnp.where(m0, a, 0.0) - jnp.where(m1, b, 0.0), axis=0, keepdims=True
            )
            part[row, 1:2, :] = jnp.sum(
                jnp.where(m1, a, 0.0) + jnp.where(m0, b, 0.0), axis=0, keepdims=True
            )

        put(0, n + C2, n + C2 + 8, [rows_of((8, count)) == c for c in range(2)])
        put(1, n, n + C2, [rows_of((C2, count)) == setting(2) * 2 + c for c in range(2)])
        put(2, 0, n, [rows_of((n, count)) == setting(2) * C2 + c * P_ + setting(3) for c in range(2)])
        fin[me_r] = part[0]
        for copy in finals(1, S - 1):
            copy.start()
        for t in range(half):
            x_copy(t).wait_send()

    def fin_wait(r):
        send(fin.at[r], fin.at[r], f_s.at[0], f_r.at[r], (1, (me_r + 1) % R)).wait_recv()

    @pl.when(me_s <= 1)
    def _():
        for d in range(1, R):
            fin_wait((me_r + d) % R)

    @pl.when(me_s > 1)
    def _():
        for r in range(R):
            fin_wait(r)

    value = fin[0]
    for r in range(1, R):
        value = value + fin[r]
    for c in range(2):
        for m in range(micro):
            out_ref[0, c, m : m + 1, :] = value[c : c + 1, m * batch : (m + 1) * batch]

    @pl.when(me_s != 1)
    def _():
        set_copy().wait_send()

    @pl.when(me_s == 0)
    def _():
        for d in range(R):
            to = (me_r + d) % R
            send(snd.at[to], uland.at[me_r], u_s.at[to], u_r.at[me_r], (1, to)).wait_send()
        for copy in finals(0, 1):
            copy.wait_send()
        for p in relayed:
            for t in range(half):
                relay(p, t).wait_send()

    @pl.when(me_s == 1)
    def _():
        for copy in finals(1, S - 1):
            copy.wait_send()

    @pl.when(me_s == 2)
    def _():
        for t in range(half):
            for e in range(2):
                v2_copy(e, t).wait_send()
            for p in range(P_):
                if p not in relayed:
                    w_copy(p, t).wait_send()
        for p in relayed:
            w_lend(p).wait_send()

    @pl.when(me_s == 3)
    def _():
        for e in range(parts):
            for d in range(R):
                v_copy(e, d).wait_send()


def local(bitstrings, boundary, stem_tensor, probe_vectors, inbound_permutations):
    S, R = lax.axis_size("section"), lax.axis_size("stem")
    rows, settings, K = stem_tensor.shape[2:]
    micro, batch, qubits = bitstrings.shape[1:]
    count = micro * batch
    C2 = 2 * settings
    n = settings * C2
    half = R // 2
    dma = pltpu.SemaphoreType.DMA
    scratch = [
        pltpu.VMEM((qubits, micro, batch), jnp.int32),
        pltpu.SMEM(boundary.shape, F32),
        pltpu.SMEM(inbound_permutations.shape, jnp.int32),
        pltpu.VMEM(inbound_permutations.shape, jnp.int32),
        pltpu.VMEM((2, K), F32),
        pltpu.VMEM((SLOTS, K // LANES, 2, STEP * settings, LANES), F32),
        pltpu.VMEM((2, 2, settings, K // BLOCK, rows, BLOCK), BF16),
        pltpu.VMEM((2, 2, settings, K // BLOCK, BLOCK, rows), BF16),
        pltpu.VMEM((K, K), BF16),
        pltpu.VMEM((2 * C2, K), jnp.int32),
        pltpu.VMEM((2 * C2 * (K // LANES), K), BF16),
        pltpu.VMEM((2, 3 * C2, K), BF16),
        pltpu.VMEM((2 * C2 * (K // LANES), LANES), BF16),
        pltpu.VMEM((C2, K), F32),
        pltpu.VMEM((C2, rows), F32),
        pltpu.VMEM((S, 8, count), F32),
        pltpu.VMEM((8, count), F32),
        pltpu.VMEM((R, C2, rows), F32),
        pltpu.VMEM((R, C2, rows), F32),
        pltpu.VMEM((R, C2, rows), F32),
        pltpu.VMEM((half, 2 * n, rows), BF16),
        pltpu.VMEM((2 * n, K), BF16),
        pltpu.VMEM((half, n, rows), F32),
        pltpu.VMEM((half, n, rows), F32),
        pltpu.VMEM((half, n, rows), F32),
        pltpu.VMEM((n, rows), F32),
        pltpu.VMEM((half, n, rows), F32),
        pltpu.VMEM((2, settings, rows), F32),
        pltpu.VMEM((half, C2, rows), F32),
        pltpu.VMEM((n + C2 + 8, n), F32),
        pltpu.VMEM((S - 1, 2, count), F32),
        pltpu.VMEM((R, 2, count), F32),
        dma((5,)),
        dma((SLOTS,)),
        dma((1,)),
        dma((S,)),
        dma((R,)),
        dma((R,)),
        dma((2 * R,)),
        dma((2 * R,)),
        dma((2 * half,)),
        dma((2 * half,)),
        dma((half,)),
        dma((half,)),
        dma((settings * half,)),
        dma((settings * half,)),
        dma((S * R,)),
        dma((R,)),
    ]
    shared = rows == BLOCK
    if shared:
        scratch.pop(7)
    out = pl.pallas_call(
        functools.partial(kernel, shared, S, R, rows, settings, K, count),
        out_shape=pltpu.VMEM((1, 2, micro, batch), F32),
        in_specs=[ANY] * 5,
        out_specs=VMEM,
        scratch_shapes=scratch,
        compiler_params=pltpu.CompilerParams(
            collective_id=1, has_side_effects=True, vmem_limit_bytes=67_000_000
        ),
    )(
        jnp.transpose(bitstrings[0], (2, 0, 1)),
        boundary,
        inbound_permutations,
        probe_vectors.reshape(2, K),
        stem_tensor.reshape(2, rows * settings, K),
    )
    return out


def solution(mesh):
    return jax.shard_map(
        local,
        mesh=mesh,
        in_specs=(
            P("section", None, None, None),
            P(),
            P("section", None, "stem", None, None),
            P("section", None, None),
            P(),
        ),
        out_specs=P("section", None, None, None),
        check_vma=False,
    )
```

```python
import functools

import jax
import jax.numpy as jnp
from jax import lax
from jax.experimental import pallas as pl
from jax.experimental.pallas import tpu as pltpu
from jax.sharding import PartitionSpec as P

MESH = pl.DeviceIdType.MESH
VMEM = pl.BlockSpec(memory_space=pltpu.VMEM)
ANY = pl.BlockSpec(memory_space=pl.ANY)
F32, BF16 = jnp.float32, jnp.bfloat16
LANES = 128
SLOTS = 5
STEP = 16
BLOCK = 256


def send(src, dst, send_sem, recv_sem, target):
    return pltpu.make_async_remote_copy(
        src_ref=src, dst_ref=dst, send_sem=send_sem, recv_sem=recv_sem, device_id=target, device_id_type=MESH
    )


def nn(a, b):
    return jnp.dot(a, b, preferred_element_type=F32)


def nt(a, b):
    return lax.dot_general(a, b, (((1,), (1,)), ((), ())), preferred_element_type=F32)


def halves(x):
    hi = x.astype(BF16)
    return hi, (x - hi.astype(F32)).astype(BF16)


def stacked(x):
    return jnp.concatenate(halves(x), axis=0)


def folded(y):
    n = y.shape[0] // 2
    return y[:n] + y[n:]


def turned(x):
    n = x.shape[0] // 2
    return jnp.concatenate([-x[n:], x[:n]], axis=0)


def rows_of(shape):
    return lax.broadcasted_iota(jnp.int32, shape, 0)


def lanes_of(shape):
    return lax.broadcasted_iota(jnp.int32, shape, 1)


def kernel(shared, S, R, rows, P_, K, count, *refs):
    refs = list(refs)
    if shared:
        refs.insert(13, refs[12])
    body(S, R, rows, P_, K, count, *refs)


def body(
    S, R, rows, P_, K, count,
    bits_hbm, bnd_hbm, perm_hbm, probe_hbm, stem_ref, out_ref,
    bits_ref, bnd_ref, perm0_ref, perm_ref, probe_ref,
    buf, hl, hlt, place, marks, masks, vecs, tails, wide, own, sets, set_own, uland, vland, snd, big, bighl, mine, other, xland, wown,
    wland, v2own, v2land, gram, part, fin,
    small_sem, load_sem, set_s, set_r, u_s, u_r, v_s, v_r, v2_s, v2_r, x_s, x_r, w_s, w_r, f_s, f_r,
):
    me_s, me_r = lax.axis_index("section"), lax.axis_index("stem")
    half = R // 2
    parity = me_r % 2
    partner = me_r + 1 - 2 * parity
    chunks = rows // STEP
    C2 = 2 * P_
    tiles = K // LANES

    block = min(rows, LANES)
    deep = block // STEP
    broad = tiles // deep
    across = tiles // broad
    turning = me_s == 2

    def load(i):
        slot = i % SLOTS
        for j in range(tiles):
            row = jnp.where(turning, (i // across) * deep + j // broad, i)
            col = jnp.where(turning, (i % across) * broad + j % broad, j)
            pltpu.make_async_copy(
                stem_ref.at[
                    :,
                    pl.ds(pl.multiple_of(row * STEP * P_, STEP * P_), STEP * P_),
                    pl.ds(pl.multiple_of(col * LANES, LANES), LANES),
                ],
                buf.at[slot, j],
                load_sem.at[slot],
            ).start()

    def loaded(slot):
        pltpu.make_async_copy(buf.at[slot], buf.at[slot], load_sem.at[slot]).wait()

    smalls = [
        pltpu.make_async_copy(src, dst, small_sem.at[e])
        for e, (src, dst) in enumerate(
            [(perm_hbm, perm_ref), (probe_hbm, probe_ref), (bits_hbm, bits_ref), (bnd_hbm, bnd_ref), (perm_hbm, perm0_ref)]
        )
    ]
    load(0)
    for copy in smalls:
        copy.start()
    for i in range(1, min(SLOTS, chunks)):
        load(i)

    barrier = pltpu.get_barrier_semaphore()
    for e in range(S):
        for d in range(R):
            if e + d:
                pl.semaphore_signal(
                    barrier, inc=1, device_id=((me_s + e) % S, (me_r + d) % R), device_id_type=MESH
                )

    own[...] = jnp.zeros_like(own)
    wide[...] = jnp.zeros_like(wide)
    for copy in smalls:
        copy.wait()

    qubits, micro, batch = bits_ref.shape
    codes = bits_ref[0].astype(F32)
    for q in range(1, qubits):
        codes = codes + float(2**q) * bits_ref[q].astype(F32)
    spread = jnp.zeros((8, count), F32)
    for m in range(micro):
        shift = (lanes_of((batch, count)) == rows_of((batch, count)) + m * batch).astype(F32).astype(BF16)
        spread = spread + nn(jnp.broadcast_to(codes[m : m + 1, :], (8, batch)).astype(BF16), shift)
    set_own[...] = spread

    blocks = tiles // chunks
    parts = 2 if rows % (2 * LANES) == 0 else 1

    def one(hit):
        return hit.astype(F32).astype(BF16)

    def columns(row):
        return jnp.broadcast_to(row, (LANES, LANES)).T

    @pl.when(me_s == 0)
    def _():
        row = perm_ref[1:2, :]
        place[0:LANES, :] = one(rows_of((LANES, K)) == row % LANES)
        marks[...] = jnp.broadcast_to(row // LANES, (2 * C2, K))

    @pl.when(me_s == 2)
    def _():
        row = perm_ref[3:4, :]
        high = jnp.broadcast_to(row // LANES, (2 * C2, K))
        for a in range(tiles):
            masks[a * 2 * C2 : (a + 1) * 2 * C2, :] = one(high == a)
        low = (row % LANES).astype(F32)
        for b in range(tiles):
            at = slice(b * LANES, (b + 1) * LANES)
            place[at, 0:LANES] = one(columns(low[:, at]) == lanes_of((LANES, LANES)).astype(F32))

    def build(i):
        for b in range(blocks):
            start = pl.multiple_of((i * blocks + b) * LANES, LANES)
            col = columns(perm_ref[2:3, pl.ds(start, LANES)].astype(F32))
            for j in range(tiles):
                target = (lanes_of((LANES, LANES)) + j * LANES).astype(F32)
                place[pl.ds(start, LANES), j * LANES : (j + 1) * LANES] = one(col == target)

    def first(i, slot):
        scal = []
        for k in range(STEP):
            at = perm0_ref[0, me_r * rows + i * STEP + k]
            scal.append((bnd_ref[0, at], bnd_ref[1, at]))
        span = 4
        for g in range(tiles // span):
            cols = [slice((g * span + t) * LANES, (g * span + t + 1) * LANES) for t in range(span)]
            a = [wide[0:P_, js] for js in cols]
            b = [wide[P_:C2, js] for js in cols]
            for k in range(STEP):
                br, bi = scal[k]
                for t in range(span):
                    tr = buf[slot, g * span + t, 0, k * P_ : (k + 1) * P_, :]
                    ti = buf[slot, g * span + t, 1, k * P_ : (k + 1) * P_, :]
                    a[t] = a[t] + (br * tr - bi * ti)
                    b[t] = b[t] + (br * ti + bi * tr)
            for t in range(span):
                wide[0:P_, cols[t]] = a[t]
                wide[P_:C2, cols[t]] = b[t]

    def against_probe(i, slot):
        width = min(rows, LANES)
        block = pl.multiple_of((i * STEP // width) * width, width)
        lane = lanes_of((P_, width))
        at = pl.ds(block, width) if rows > width else slice(None)
        a, b = own[0:P_, at], own[P_:C2, at]
        for k in range(STEP):
            ar = jnp.zeros((P_, LANES), F32)
            ai = jnp.zeros((P_, LANES), F32)
            for j in range(tiles):
                js = slice(j * LANES, (j + 1) * LANES)
                tr = buf[slot, j, 0, k * P_ : (k + 1) * P_, :]
                ti = buf[slot, j, 1, k * P_ : (k + 1) * P_, :]
                pr, pi = wide[0:P_, js], wide[P_:C2, js]
                ar = ar + (tr * pr - ti * pi)
                ai = ai + (tr * pi + ti * pr)
            hit = lane == (i * STEP + k - block)
            a = jnp.where(hit, jnp.sum(ar, axis=1, keepdims=True), a)
            b = jnp.where(hit, jnp.sum(ai, axis=1, keepdims=True), b)
        own[0:P_, at] = a
        own[P_:C2, at] = b

    def split(i, slot):
        at = pl.ds(pl.multiple_of(i * STEP, STEP), STEP)

        def column(j, carry):
            js = pl.ds(pl.multiple_of(j % (BLOCK // LANES) * LANES, LANES), LANES)
            for c in range(2):
                for p in range(P_):
                    hi, lo = halves(buf[slot, j, c, pl.ds(p, STEP, P_), :])
                    hl[c, 0, p, j // (BLOCK // LANES), at, js] = hi
                    hl[c, 1, p, j // (BLOCK // LANES), at, js] = lo
            return carry

        lax.fori_loop(0, tiles, column, 0)

    def split_turned(i, slot):
        at = pl.ds(pl.multiple_of(i // across * block, block), block) if rows > block else slice(None)

        def column(e, carry):
            j, c = e // 2, e % 2
            tile = (i % across) * broad + j
            js = pl.ds(pl.multiple_of(tile % (BLOCK // LANES) * LANES, LANES), LANES)
            for p in range(P_):
                x = [buf[slot, d * broad + j, c, pl.ds(p, STEP, P_), :] for d in range(deep)]
                hi, lo = halves(jnp.concatenate(x, axis=0).T)
                hlt[c, 0, p, tile // (BLOCK // LANES), js, at] = hi
                hlt[c, 1, p, tile // (BLOCK // LANES), js, at] = lo
            return carry

        lax.fori_loop(0, 2 * broad, column, 0)

    @pl.when(me_s == 3)
    def _():
        wide[0:P_, :] = jnp.broadcast_to(probe_ref[0:1, :], (P_, K))
        wide[P_:C2, :] = jnp.broadcast_to(probe_ref[1:2, :], (P_, K))

    def stream(i, carry):
        slot = i % SLOTS
        loaded(slot)

        @pl.when(me_s == 0)
        def _():
            first(i, slot)

        @pl.when(me_s == 1)
        def _():
            build(i)
            split(i, slot)

        @pl.when(me_s == 2)
        def _():
            split_turned(i, slot)

        @pl.when(me_s == 3)
        def _():
            against_probe(i, slot)

        @pl.when(i + SLOTS < chunks)
        def _():
            load(i + SLOTS)

        return carry

    def v_copy(e, d):
        to = (me_r + d) % R
        n = rows // parts
        at = (slice(None), pl.ds(e * n, n))
        return send(own.at[at], vland.at[(me_r,) + at], v_s.at[e * R + d], v_r.at[me_r * parts + e], (2, to))

    for e in range(parts):
        lax.fori_loop(e * (chunks // parts), (e + 1) * (chunks // parts), stream, 0)
        if e == 0:
            pl.semaphore_wait(barrier, S * R - 1)

        @pl.when(me_s == 3)
        def _():
            for d in range(R):
                v_copy(e, d).start()

    def set_copy():
        return send(set_own, sets.at[me_s], set_s.at[0], set_r.at[me_s], (1, me_r))

    def set_wait(s):
        send(sets.at[s], sets.at[s], set_s.at[0], set_r.at[s], (0, me_r)).wait_recv()

    @pl.when(me_s != 1)
    def _():
        set_copy().start()

    def finals(section, lo):
        return [
            send(part.at[e], fin.at[me_r], f_s.at[e * R + d], f_r.at[me_r], (section + e, (me_r + d) % R))
            for e in range(lo)
            for d in range(R)
            if e + d
        ]

    setting = lambda s: sets[s, 0:1, :].astype(jnp.int32)

    @pl.when(me_s == 0)
    def _():
        u = stacked(wide[...])
        tall = jnp.concatenate([u[:, a * LANES : (a + 1) * LANES] for a in range(tiles)], axis=0)
        span = max(rows, LANES)

        def spot(d, carry):
            step = (me_r * rows // span + d) % (K // span)
            at = pl.ds(pl.multiple_of(step * span, span), span)
            z = nn(tails[...], place[0:LANES, at])
            mark = marks[:, at]
            got = z[0 : 2 * C2]
            for a in range(1, tiles):
                got = jnp.where(mark == a, z[a * 2 * C2 : (a + 1) * 2 * C2], got)
            got = folded(got)
            for e in range(span // rows):
                to = step * (span // rows) + e
                snd[to] = got[:, e * rows : (e + 1) * rows]
                send(snd.at[to], uland.at[me_r], u_s.at[to], u_r.at[me_r], (1, to)).start()
            return carry

        tails[...] = tall
        lax.fori_loop(0, K // span, spot, 0)
        ur, ui = wide[0:P_, :], wide[P_:C2, :]
        pr, pi = probe_ref[0:1, :], probe_ref[1:2, :]
        hit = rows_of((P_, count)) == set_own[0:1, :].astype(jnp.int32)
        re = jnp.sum(ur * pr - ui * pi, axis=1, keepdims=True)
        im = jnp.sum(ur * pi + ui * pr, axis=1, keepdims=True)
        part[0, 0:1, :] = jnp.sum(jnp.where(hit, re, 0.0), axis=0, keepdims=True)
        part[0, 1:2, :] = jnp.sum(jnp.where(hit, im, 0.0), axis=0, keepdims=True)
        fin[me_r] = part[0]
        for copy in finals(0, 1):
            copy.start()

    mid = P_ // 2
    relayed = [q + q // (mid - 1) for q in range(mid)]
    spot = me_r // 2

    def w_rows(p):
        return pl.ds(pl.multiple_of(p * C2, C2), C2)

    def w_copy(p, t):
        at, to = w_rows(p), (me_r + 2 * t) % R
        return send(wown.at[at], wland.at[spot, at], w_s.at[p * half + t], w_r.at[spot * P_ + p], (1, to))

    def w_lend(p):
        at = w_rows(p)
        return send(wown.at[at], wland.at[spot, at], w_s.at[p * half], w_r.at[spot * P_ + p], (0, me_r))

    def relay(p, t):
        at, to = (spot, w_rows(p)), (me_r + 2 * t) % R
        return send(wland.at[at], wland.at[at], w_s.at[p * half + t], w_r.at[spot * P_ + p], (1, to))

    def w_wait(p, t):
        at = (t, w_rows(p))
        send(wland.at[at], wland.at[at], w_s.at[p * half], w_r.at[t * P_ + p], (2, me_r)).wait_recv()

    def v2_copy(e, t):
        to = (me_r + 2 * t) % R
        at = pl.ds(pl.multiple_of(e * P_, P_), P_)
        return send(v2own.at[e], v2land.at[me_r // 2, at], v2_s.at[e * half + t], v2_r.at[(me_r // 2) * 2 + e], (1, to))

    @pl.when(me_s == 0)
    def _():
        def hop(q, carry):
            p = q + q // (mid - 1)
            w_wait(p, spot)
            for t in range(half):
                relay(p, t).start()
            return carry

        lax.fori_loop(0, mid, hop, 0)

    @pl.when(me_s == 2)
    def _():
        for r in range(R):
            for e in range(parts):
                n = rows // parts
                at = vland.at[r, :, pl.ds(e * n, n)]
                send(at, at, v_s.at[0], v_r.at[r * parts + e], (3, me_r)).wait_recv()
        z = None
        for r in range(R):
            at = slice(r * rows, (r + 1) * rows)
            v = stacked(vland[r])
            tall = jnp.concatenate(
                [masks[a * 2 * C2 : (a + 1) * 2 * C2, at] * v for a in range(tiles)], axis=0
            )
            y = nn(tall, place[at, 0:LANES])
            z = y if z is None else z + y
        y = jnp.concatenate([z[a * 2 * C2 : (a + 1) * 2 * C2] for a in range(tiles)], axis=1)
        hi, lo = y[:C2], y[C2:]
        probe = probe_ref[...]

        def ends(x):
            return [h.astype(F32) for h in halves(jnp.concatenate([x] * (P_ // 2), axis=0))]

        straight = jnp.concatenate([hi, lo] + ends(probe), axis=0).astype(BF16)
        crossed = jnp.concatenate([turned(hi), turned(lo)] + ends(turned(probe)), axis=0).astype(BF16)
        vecs[0] = straight
        vecs[1] = crossed
        v2own[...] = jnp.zeros_like(v2own)

        def back(pair, carry):
            for odd in range(2):
                p = 2 * pair + odd
                z = None
                for c in range(2):
                    for h in range(2):
                        for b in range(K // BLOCK):
                            y = nn(vecs[c, :, b * BLOCK : (b + 1) * BLOCK], hlt[c, h, p, b])
                            z = y if z is None else z + y
                wown[pl.ds(pl.multiple_of(p * C2, C2), C2), :] = folded(z[: 2 * C2])
                e = p // (P_ // 2)
                v2own[e] = jnp.where(rows_of((P_, rows)) // 2 == p % (P_ // 2), folded(z[2 * C2 :]), v2own[e])

            @pl.when((pair + 1) % (P_ // 4) == 0)
            def _():
                for t in range(half):
                    v2_copy(pair // (P_ // 4), t).start()

            for odd in range(2):
                p = 2 * pair + odd
                lent = jnp.logical_or(p < mid - 1, p == mid)

                @pl.when(lent)
                def _():
                    w_lend(p).start()

                @pl.when(jnp.logical_not(lent))
                def _():
                    for t in range(half):
                        w_copy(p, t).start()

            return carry

        lax.fori_loop(0, P_ // 2, back, 0)

    @pl.when(me_s == 1)
    def _():
        for r in range(R):
            send(uland.at[r], uland.at[r], u_s.at[0], u_r.at[r], (0, me_r)).wait_recv()
        x = uland[0]
        for r in range(1, R):
            x = x + uland[r]
        straight, crossed = stacked(x), stacked(turned(x))

        def front(p, carry):
            for b in range(K // BLOCK):
                z = nn(straight, hl[0, 0, p, b]) + nn(crossed, hl[1, 0, p, b])
                z = z + nn(straight, hl[0, 1, p, b]) + nn(crossed, hl[1, 1, p, b])
                hi, lo = halves(folded(z))
                js = slice(b * BLOCK, (b + 1) * BLOCK)
                bighl[pl.ds(pl.multiple_of(p * C2, C2), C2), js] = hi
                bighl[pl.ds(pl.multiple_of(P_ * C2 + p * C2, C2), C2), js] = lo
            return carry

        lax.fori_loop(0, P_, front, 0)
        n = P_ * C2

        def shuffled(q):
            return folded(nt(bighl[...], place[pl.ds(pl.multiple_of(q * rows, rows), rows), :]))

        def x_copy(t):
            return send(other.at[t], xland.at[t], x_s.at[t], x_r.at[t], (1, partner))

        def give(t, carry):
            other[t] = shuffled(2 * t + 1 - parity)
            x_copy(t).start()
            return carry

        def keep(t, carry):
            mine[t] = shuffled(2 * t + parity)
            return carry

        lax.fori_loop(0, half, give, 0)
        lax.fori_loop(0, half, keep, 0)
        probes = jnp.concatenate([probe_ref[...], jnp.zeros((6, K), F32)], axis=0)
        g1 = folded(nt(stacked(probes), bighl[...]))
        gram[n + C2 : n + C2 + 8, :] = g1[:, :n] + g1[:, n:]
        sets[1] = set_own[...]
        for s in (0, 2, 3):
            set_wait(s)
        hits = [rows_of((n, count)) == setting(1) * C2 + c * P_ + setting(0) for c in range(2)]
        pick = jnp.concatenate([h.astype(F32) for h in hits], axis=1).astype(BF16)

        for t in range(half):
            x_copy(t).wait_recv()
            hi, lo = halves(mine[t] + xland[t])
            big[t, 0:n, :] = hi
            big[t, n : 2 * n, :] = lo

        def inner(q, carry):
            p = q
            at = pl.ds(pl.multiple_of(p * C2, C2), C2)
            for t in range(half):
                w_wait(p, t)
            acc = nt(stacked(wland[0, at, :]), big[0])
            for t in range(1, half):
                acc = acc + nt(stacked(wland[t, at, :]), big[t])
            acc = folded(acc)
            gram[at, :] = acc[:, :n] + acc[:, n:]
            return carry

        lax.fori_loop(0, P_ - 1, inner, 0)
        acc = None
        for t in range(half):
            for e in range(2):
                at = v2land.at[t, pl.ds(e * P_, P_)]
                send(at, at, v2_s.at[0], v2_r.at[t * 2 + e], (2, me_r)).wait_recv()
            got = nt(stacked(v2land[t]), big[t])
            acc = got if acc is None else acc + got
        acc = folded(acc)
        gram[n : n + C2, :] = acc[:, :n] + acc[:, n:]
        lax.fori_loop(P_ - 1, P_, inner, 0)

        y = folded(nn(stacked(gram[...]), pick))
        y0, y1 = y[:, :count], y[:, count:]

        def put(row, lo, hi, masks):
            a, b = y0[lo:hi], y1[lo:hi]
            m0, m1 = masks
            part[row, 0:1, :] = jnp.sum(
                jnp.where(m0, a, 0.0) - jnp.where(m1, b, 0.0), axis=0, keepdims=True
            )
            part[row, 1:2, :] = jnp.sum(
                jnp.where(m1, a, 0.0) + jnp.where(m0, b, 0.0), axis=0, keepdims=True
            )

        put(0, n + C2, n + C2 + 8, [rows_of((8, count)) == c for c in range(2)])
        put(1, n, n + C2, [rows_of((C2, count)) == setting(2) * 2 + c for c in range(2)])
        put(2, 0, n, [rows_of((n, count)) == setting(2) * C2 + c * P_ + setting(3) for c in range(2)])
        fin[me_r] = part[0]
        for copy in finals(1, S - 1):
            copy.start()
        for t in range(half):
            x_copy(t).wait_send()

    def fin_wait(r):
        send(fin.at[r], fin.at[r], f_s.at[0], f_r.at[r], (1, (me_r + 1) % R)).wait_recv()

    @pl.when(me_s <= 1)
    def _():
        for d in range(1, R):
            fin_wait((me_r + d) % R)

    @pl.when(me_s > 1)
    def _():
        for r in range(R):
            fin_wait(r)

    value = fin[0]
    for r in range(1, R):
        value = value + fin[r]
    for c in range(2):
        for m in range(micro):
            out_ref[0, c, m : m + 1, :] = value[c : c + 1, m * batch : (m + 1) * batch]

    @pl.when(me_s != 1)
    def _():
        set_copy().wait_send()

    @pl.when(me_s == 0)
    def _():
        for d in range(R):
            to = (me_r + d) % R
            send(snd.at[to], uland.at[me_r], u_s.at[to], u_r.at[me_r], (1, to)).wait_send()
        for copy in finals(0, 1):
            copy.wait_send()
        for p in relayed:
            for t in range(half):
                relay(p, t).wait_send()

    @pl.when(me_s == 1)
    def _():
        for copy in finals(1, S - 1):
            copy.wait_send()

    @pl.when(me_s == 2)
    def _():
        for t in range(half):
            for e in range(2):
                v2_copy(e, t).wait_send()
            for p in range(P_):
                if p not in relayed:
                    w_copy(p, t).wait_send()
        for p in relayed:
            w_lend(p).wait_send()

    @pl.when(me_s == 3)
    def _():
        for e in range(parts):
            for d in range(R):
                v_copy(e, d).wait_send()


def local(bitstrings, boundary, stem_tensor, probe_vectors, inbound_permutations):
    S, R = lax.axis_size("section"), lax.axis_size("stem")
    rows, settings, K = stem_tensor.shape[2:]
    micro, batch, qubits = bitstrings.shape[1:]
    count = micro * batch
    C2 = 2 * settings
    n = settings * C2
    half = R // 2
    dma = pltpu.SemaphoreType.DMA
    scratch = [
        pltpu.VMEM((qubits, micro, batch), jnp.int32),
        pltpu.SMEM(boundary.shape, F32),
        pltpu.SMEM(inbound_permutations.shape, jnp.int32),
        pltpu.VMEM(inbound_permutations.shape, jnp.int32),
        pltpu.VMEM((2, K), F32),
        pltpu.VMEM((SLOTS, K // LANES, 2, STEP * settings, LANES), F32),
        pltpu.VMEM((2, 2, settings, K // BLOCK, rows, BLOCK), BF16),
        pltpu.VMEM((2, 2, settings, K // BLOCK, BLOCK, rows), BF16),
        pltpu.VMEM((K, K), BF16),
        pltpu.VMEM((2 * C2, K), jnp.int32),
        pltpu.VMEM((2 * C2 * (K // LANES), K), BF16),
        pltpu.VMEM((2, 3 * C2, K), BF16),
        pltpu.VMEM((2 * C2 * (K // LANES), LANES), BF16),
        pltpu.VMEM((C2, K), F32),
        pltpu.VMEM((C2, rows), F32),
        pltpu.VMEM((S, 8, count), F32),
        pltpu.VMEM((8, count), F32),
        pltpu.VMEM((R, C2, rows), F32),
        pltpu.VMEM((R, C2, rows), F32),
        pltpu.VMEM((R, C2, rows), F32),
        pltpu.VMEM((half, 2 * n, rows), BF16),
        pltpu.VMEM((2 * n, K), BF16),
        pltpu.VMEM((half, n, rows), F32),
        pltpu.VMEM((half, n, rows), F32),
        pltpu.VMEM((half, n, rows), F32),
        pltpu.VMEM((n, rows), F32),
        pltpu.VMEM((half, n, rows), F32),
        pltpu.VMEM((2, settings, rows), F32),
        pltpu.VMEM((half, C2, rows), F32),
        pltpu.VMEM((n + C2 + 8, n), F32),
        pltpu.VMEM((S - 1, 2, count), F32),
        pltpu.VMEM((R, 2, count), F32),
        dma((5,)),
        dma((SLOTS,)),
        dma((1,)),
        dma((S,)),
        dma((R,)),
        dma((R,)),
        dma((2 * R,)),
        dma((2 * R,)),
        dma((2 * half,)),
        dma((2 * half,)),
        dma((half,)),
        dma((half,)),
        dma((settings * half,)),
        dma((settings * half,)),
        dma((S * R,)),
        dma((R,)),
    ]
    shared = rows == BLOCK
    if shared:
        scratch.pop(7)
    out = pl.pallas_call(
        functools.partial(kernel, shared, S, R, rows, settings, K, count),
        out_shape=pltpu.VMEM((1, 2, micro, batch), F32),
        in_specs=[ANY] * 5,
        out_specs=VMEM,
        scratch_shapes=scratch,
        compiler_params=pltpu.CompilerParams(
            collective_id=1, has_side_effects=True, vmem_limit_bytes=67_000_000
        ),
    )(
        jnp.transpose(bitstrings[0], (2, 0, 1)),
        boundary,
        inbound_permutations,
        probe_vectors.reshape(2, K),
        stem_tensor.reshape(2, rows * settings, K),
    )
    return out


def solution(mesh):
    return jax.shard_map(
        local,
        mesh=mesh,
        in_specs=(
            P("section", None, None, None),
            P(),
            P("section", None, "stem", None, None),
            P("section", None, None),
            P(),
        ),
        out_specs=P("section", None, None, None),
        check_vma=False,
    )
```
